8 devices in a mesh: node: 2 (over z, y), data: 4 (over x, core).
Axes of the slice: x: 2, y: 2, z: 1, core: 2. Of those that a mesh axis runs over, the one named last changes fastest.
Arguments:
- tokens: bfloat16 [65536, 768], P(('node', 'data'))
- grad_out: bfloat16 [65536, 768], P(('node', 'data'))
- weights: bfloat16 [8, 768, 768], replicated
- a_old: float32 [8, 768, 768], replicated
- s_old: float32 [8, 768, 768], replicated
- a_inv: float32 [8, 768, 768], replicated
- s_inv: float32 [8, 768, 768], replicated
Outputs:
- output 1: float32 [8, 768, 768], replicated
- output 2: float32 [8, 768, 768], replicated
- output 3: float32 [8, 768, 768], replicated
All inputs are finite; a program needn't handle non-finite values.
Results may differ from the reference program's by a relative error of at most 0.00149.
Values are sent between devices in bfloat16 or wider.
A program may use at most 1 GiB of HBM per device.

```python
import jax
import jax.numpy as jnp
from jax import lax

D = 768
LAYERS = 8
TOKENS_DEV = 8192
SHARDS = 8
TOKENS_ALL = SHARDS * TOKENS_DEV
FACTOR_DECAY = 0.8
GELU_SCALE = 0.7978845608028654
GELU_CUBIC = 0.044715


def spd_draw(rng_key):
    key_diag, key_low = jax.random.split(rng_key)
    diagonal = jax.random.uniform(key_diag, (LAYERS, D), jnp.float32, 0.5, 1.5)
    low_part = jax.random.normal(key_low, (LAYERS, D, 64), jnp.float32) * D ** -0.5
    low_sq = jnp.einsum('lir,ljr->lij', low_part, low_part)
    return low_sq + diagonal[:, :, None] * jnp.eye(D, dtype=jnp.float32)


def draw_side(key_noise, key_scale, key_shift, shift_size):
    noise = jax.random.normal(key_noise, (SHARDS, TOKENS_DEV, D), jnp.float32)
    shard_scale = jax.random.uniform(key_scale, (SHARDS, 1, 1), jnp.float32, 0.5, 1.5)
    shard_shift = shift_size * jax.random.normal(key_shift, (SHARDS, 1, D), jnp.float32)
    return (noise * shard_scale + shard_shift).reshape(TOKENS_ALL, D).astype(jnp.bfloat16)


def setup_inputs(seed: int = 0) -> dict:
    keys = jax.random.split(jax.random.key(seed), 11)
    tokens = draw_side(keys[0], keys[1], keys[2], 0.7)
    grad_out = draw_side(keys[3], keys[4], keys[5], 0.7)
    weights = (1.5 * D ** -0.5 * jax.random.normal(keys[6], (LAYERS, D, D), jnp.float32)).astype(jnp.bfloat16)
    return {'tokens': tokens, 'grad_out': grad_out, 'weights': weights, 'a_old': spd_draw(keys[7]), 's_old': spd_draw(keys[8]), 'a_inv': spd_draw(keys[9]), 's_inv': spd_draw(keys[10])}


def gelu_value(pre_act):
    pre_f = pre_act.astype(jnp.float32)
    return 0.5 * pre_f * (1.0 + jnp.tanh(GELU_SCALE * (pre_f + GELU_CUBIC * pre_f * pre_f * pre_f)))


def gelu_slope(pre_act):
    pre_f = pre_act.astype(jnp.float32)
    tanh_val = jnp.tanh(GELU_SCALE * (pre_f + GELU_CUBIC * pre_f * pre_f * pre_f))
    return 0.5 * (1.0 + tanh_val) + 0.5 * pre_f * (1.0 - tanh_val * tanh_val) * GELU_SCALE * (1.0 + 3.0 * GELU_CUBIC * pre_f * pre_f)


def shard_terms(tok_rows, dout_rows, weights):
    hidden = [tok_rows]
    pre_list = []
    for layer in range(LAYERS - 1):
        pre_act = jnp.dot(hidden[layer], weights[layer], preferred_element_type=jnp.float32).astype(jnp.bfloat16)
        pre_list.append(pre_act)
        hidden.append(gelu_value(pre_act).astype(jnp.bfloat16))
    w_parts = []
    a_parts = []
    s_parts = []
    grad_h = dout_rows
    for layer in reversed(range(LAYERS)):
        if layer == LAYERS - 1:
            grad_pre = grad_h
        else:
            grad_pre = (grad_h.astype(jnp.float32) * gelu_slope(pre_list[layer])).astype(jnp.bfloat16)
        w_parts.append(jnp.dot(hidden[layer].T, grad_pre, preferred_element_type=jnp.float32))
        a_parts.append(jnp.dot(hidden[layer].T, hidden[layer], preferred_element_type=jnp.float32))
        s_parts.append(jnp.dot(grad_pre.T, grad_pre, preferred_element_type=jnp.float32))
        if layer > 0:
            grad_h = jnp.dot(grad_pre, weights[layer].T, preferred_element_type=jnp.float32).astype(jnp.bfloat16)
    return (jnp.stack(w_parts[::-1]), jnp.stack(a_parts[::-1]), jnp.stack(s_parts[::-1]))


def reference(tokens, grad_out, weights, a_old, s_old, a_inv, s_inv):
    tok_blocks = tokens.reshape(SHARDS, TOKENS_DEV, D)
    dout_blocks = grad_out.reshape(SHARDS, TOKENS_DEV, D)

    def accumulate(totals, block_pair):
        pieces = shard_terms(block_pair[0], block_pair[1], weights)
        return tuple(total + piece for total, piece in zip(totals, pieces)), None

    zero_stack = jnp.zeros((LAYERS, D, D), jnp.float32)
    sums = lax.scan(accumulate, (zero_stack, zero_stack, zero_stack), (tok_blocks, dout_blocks))[0]
    grad_w = sums[0] / TOKENS_ALL
    a_cur = sums[1] / TOKENS_ALL
    s_cur = sums[2] / TOKENS_ALL
    a_new = FACTOR_DECAY * a_old + (1.0 - FACTOR_DECAY) * a_cur
    s_new = FACTOR_DECAY * s_old + (1.0 - FACTOR_DECAY) * s_cur
    left = jnp.einsum('lij,ljk->lik', a_inv.astype(jnp.float32), grad_w.astype(jnp.float32))
    update = jnp.einsum('lij,ljk->lik', left, s_inv.astype(jnp.float32))
    return (update, a_new, s_new)
```

```python
import functools
import jax
import jax.numpy as jnp
from jax import lax
from jax.experimental import pallas as pl
from jax.experimental.pallas import tpu as pltpu
from jax.sharding import PartitionSpec as P

FACTOR_DECAY = 0.8
GELU_SCALE = 0.7978845608028654
GELU_CUBIC = 0.044715
D = 768
B = 256
TILE = 1024
SUB = 256


def tn(left, right):
    return lax.dot_general(left, right, (((0,), (0,)), ((), ())), preferred_element_type=jnp.float32)


def nt(left, right):
    return lax.dot_general(left, right, (((1,), (1,)), ((), ())), preferred_element_type=jnp.float32)


def gelu_parts(pre_act):
    z = pre_act.astype(jnp.float32)
    q = (GELU_CUBIC * z) * z
    gz = GELU_SCALE * z
    t = jnp.tanh(gz + gz * q)
    hz = 0.5 * z
    return q, t, hz


def gelu_value(pre_act):
    _, t, hz = gelu_parts(pre_act)
    return (hz + hz * t).astype(jnp.bfloat16)


def gelu_both(pre_act):
    q, t, hz = gelu_parts(pre_act)
    slope = (0.5 + 0.5 * t) + (hz * (1.0 - t * t)) * (GELU_SCALE + (3.0 * GELU_SCALE) * q)
    return (hz + hz * t).astype(jnp.bfloat16), slope


def gram_add(acc, x):
    acc[0:B, :] += tn(x[:, 0:B], x)
    acc[B:2 * B, 0:2 * B] += tn(x[:, B:2 * B], x[:, B:])
    acc[B:2 * B, 2 * B:] += tn(x[:, 2 * B:], x[:, 2 * B:])


def fwd_kernel(n_tiles, layers, tok_ref, w_ref, z_ref, a_ref, h_s):
    l = pl.program_id(0)
    t = pl.program_id(1)

    @pl.when(l == 0)
    def _():
        h_s[t] = tok_ref[...]

    @pl.when(t == 0)
    def _():
        a_ref[...] = jnp.zeros_like(a_ref)

    @pl.when(l < layers - 1)
    def _():
        x = h_s[t]
        for r in range(0, TILE, SUB):
            for c in range(0, D, B):
                z = jnp.dot(x[r:r + SUB, :], w_ref[0, :, c:c + B], preferred_element_type=jnp.float32).astype(jnp.bfloat16)
                z_ref[0, r:r + SUB, c:c + B] = z
                h_s[t, r:r + SUB, c:c + B] = gelu_value(z)
        gram_add(a_ref.at[0], x)

    @pl.when(l == layers - 1)
    def _():
        gram_add(a_ref.at[0], h_s[t])


def bwd_kernel(n_tiles, first, count, dout_ref, z_ref, tok_ref, w_ref, s_ref, g_ref, gout_ref, g_s):
    i = pl.program_id(0)
    t = pl.program_id(1)

    @pl.when(i == 0)
    def _():
        g_s[t] = dout_ref[...]

    @pl.when(t == 0)
    def _():
        s_ref[...] = jnp.zeros_like(s_ref)
        g_ref[...] = jnp.zeros_like(g_ref)

    def inner():
        g = g_s[t]
        z = z_ref[0]
        h, slope = gelu_both(z)
        for r in range(0, TILE, SUB):
            for c in range(0, D, B):
                dh = nt(g[r:r + SUB, :], w_ref[0, c:c + B, :]).astype(jnp.bfloat16)
                g_s[t, r:r + SUB, c:c + B] = (dh.astype(jnp.float32) * slope[r:r + SUB, c:c + B]).astype(jnp.bfloat16)
        for m in range(0, D, B):
            g_ref[0, m:m + B, :] += tn(g[:, m:m + B], h)
        gram_add(s_ref.at[0], g)
        gout_ref[...] = g_s[t]

    def last():
        g = g_s[t]
        h = tok_ref[...]
        for m in range(0, D, B):
            g_ref[0, m:m + B, :] += tn(g[:, m:m + B], h)
        gram_add(s_ref.at[0], g)
        gout_ref[...] = g

    final = first - (count - 1) == 0
    if final:
        pl.when(i < count - 1)(inner)
        pl.when(i == count - 1)(last)
    else:
        inner()


def forward(tok, w):
    n, d = tok.shape
    layers = w.shape[0]
    nt_ = n // TILE
    z_map = lambda l, t: (jnp.minimum(l, layers - 2), jnp.where(l < layers - 1, t, nt_ - 1), 0)
    return pl.pallas_call(
        functools.partial(fwd_kernel, nt_, layers),
        grid=(layers, nt_),
        in_specs=[
            pl.BlockSpec((TILE, d), lambda l, t: (jnp.where(l == 0, t, nt_ - 1), 0)),
            pl.BlockSpec((1, d, d), lambda l, t: (jnp.minimum(l, layers - 2), 0, 0)),
        ],
        out_specs=[
            pl.BlockSpec((1, TILE, d), z_map),
            pl.BlockSpec((1, 2 * B, d), lambda l, t: (l, 0, 0)),
        ],
        out_shape=[
            jax.ShapeDtypeStruct((layers - 1, n, d), jnp.bfloat16),
            jax.ShapeDtypeStruct((layers, 2 * B, d), jnp.float32),
        ],
        scratch_shapes=[pltpu.VMEM((nt_, TILE, d), jnp.bfloat16)],
        compiler_params=pltpu.CompilerParams(vmem_limit_bytes=60 * 2 ** 20),
        cost_estimate=pl.CostEstimate(flops=int(layers * 2 * n * d * d * 1.6), bytes_accessed=100 * 2 ** 20, transcendentals=0),
        name="fwd_stack",
    )(tok, w)


def backward(dout, z, tok, w, first, count):
    n, d = tok.shape
    nt_ = n // TILE
    lay = lambda i: first - i
    return pl.pallas_call(
        functools.partial(bwd_kernel, nt_, first, count),
        grid=(count, nt_),
        in_specs=[
            pl.BlockSpec((TILE, d), lambda i, t: (jnp.where(i == 0, t, nt_ - 1), 0)),
            pl.BlockSpec((1, TILE, d), lambda i, t: (jnp.maximum(lay(i) - 1, 0), jnp.where(lay(i) > 0, t, nt_ - 1), 0)),
            pl.BlockSpec((TILE, d), lambda i, t: (jnp.where(lay(i) == 0, t, 0), 0)),
            pl.BlockSpec((1, d, d), lambda i, t: (lay(i), 0, 0)),
        ],
        out_specs=[
            pl.BlockSpec((1, 2 * B, d), lambda i, t: (i, 0, 0)),
            pl.BlockSpec((1, d, d), lambda i, t: (i, 0, 0)),
            pl.BlockSpec((TILE, d), lambda i, t: (jnp.where(i == count - 1, t, 0), 0)),
        ],
        out_shape=[
            jax.ShapeDtypeStruct((count, 2 * B, d), jnp.float32),
            jax.ShapeDtypeStruct((count, d, d), jnp.float32),
            jax.ShapeDtypeStruct((n, d), jnp.bfloat16),
        ],
        scratch_shapes=[pltpu.VMEM((nt_, TILE, d), jnp.bfloat16)],
        compiler_params=pltpu.CompilerParams(vmem_limit_bytes=60 * 2 ** 20),
        cost_estimate=pl.CostEstimate(flops=int(count * 2 * n * d * d * 2.7), bytes_accessed=100 * 2 ** 20, transcendentals=0),
        name="bwd_stack",
    )(dout, z, tok, w)


def unpack(p):
    b00, b01, b02 = p[:, 0:B, 0:B], p[:, 0:B, B:2 * B], p[:, 0:B, 2 * B:]
    b11, b12, b22 = p[:, B:, 0:B], p[:, B:, B:2 * B], p[:, B:, 2 * B:]
    tr = lambda x: jnp.swapaxes(x, 1, 2)
    return jnp.concatenate([
        jnp.concatenate([b00, b01, b02], 2),
        jnp.concatenate([tr(b01), b11, b12], 2),
        jnp.concatenate([tr(b02), tr(b12), b22], 2)], 1)


CHUNKS = ((7, 2), (5, 2), (3, 2), (1, 2))


def solution(mesh):
    batch_axes = ('node', 'data')
    row_spec = P(batch_axes, None)
    full_spec = P()

    def kfac_step(tokens, grad_out, weights, a_old, s_old, a_inv, s_inv):
        inv_total = 1.0 / tokens.shape[0]

        def per_device(tok, dout, w, a_prev, s_prev, a_pre, s_pre):
            z, a_loc = forward(tok, w)
            a_sum = lax.psum(a_loc, batch_axes)
            s_list, g_list = [], []
            g = dout
            for first, count in CHUNKS:
                s_loc, g_loc, g = backward(g, z, tok, w, first, count)
                s_sum, g_sum = lax.psum((s_loc, g_loc), batch_axes)
                s_list.append(s_sum[::-1])
                g_list.append(g_sum[::-1])
            s_sum = jnp.concatenate(s_list[::-1], 0)
            gt_sum = jnp.concatenate(g_list[::-1], 0) * inv_total
            a_new = FACTOR_DECAY * a_prev + (1.0 - FACTOR_DECAY) * (unpack(a_sum) * inv_total)
            s_new = FACTOR_DECAY * s_prev + (1.0 - FACTOR_DECAY) * (unpack(s_sum) * inv_total)
            me = lax.axis_index('node') * lax.axis_size('data') + lax.axis_index('data')
            take = lambda x: lax.dynamic_slice_in_dim(x, me, 1, 0)[0]
            hi = lax.Precision.HIGHEST
            left = lax.dot_general(take(a_pre), take(gt_sum), (((1,), (1,)), ((), ())), precision=hi, preferred_element_type=jnp.float32)
            upd = jnp.dot(left, take(s_pre), precision=hi, preferred_element_type=jnp.float32)
            update = lax.all_gather(upd, batch_axes)
            return update, a_new, s_new

        return jax.shard_map(per_device, mesh=mesh, in_specs=(row_spec, row_spec, full_spec, full_spec, full_spec, full_spec, full_spec), out_specs=(full_spec, full_spec, full_spec), check_vma=False)(tokens, grad_out, weights, a_old, s_old, a_inv, s_inv)

    return kfac_step
```

```python
import functools
import jax
import jax.numpy as jnp
from jax import lax
from jax.experimental import pallas as pl
from jax.experimental.pallas import tpu as pltpu
from jax.sharding import PartitionSpec as P

FACTOR_DECAY = 0.8
GELU_SCALE = 0.7978845608028654
GELU_CUBIC = 0.044715
D = 768
B = 256
NT = 8
DEV = 8
AR = 64
GR = 96
SR = AR + GR
L = 8
MESH = pl.DeviceIdType.MESH
T1, T2, T3, T4, T5, T6, T7 = 0, 1, 5, 7, 1, 5, 7


def tn(left, right):
    return lax.dot_general(left, right, (((0,), (0,)), ((), ())), preferred_element_type=jnp.float32)


def nt(left, right):
    return lax.dot_general(left, right, (((1,), (1,)), ((), ())), preferred_element_type=jnp.float32)


def half_parts(half_act):
    y = half_act.astype(jnp.float32)
    sq = jnp.minimum(y * y, 1e37)
    kp = (8.0 * GELU_SCALE * GELU_CUBIC) * sq
    a = 2.0 * GELU_SCALE + kp
    return y, kp, a, jnp.tanh(y * a)


def gelu_value(half_act):
    y, _, _, t = half_parts(half_act)
    return (y + y * t).astype(jnp.bfloat16)


def gelu_both(half_act):
    y, kp, a, t = half_parts(half_act)
    opt = 1.0 + t
    h = y * opt
    slope2 = opt + (h * (1.0 - t)) * ((a + kp) + kp)
    return h.astype(jnp.bfloat16), slope2


def add_rows(acc, p, base, rows, first, c0, val):
    n = val.shape[0]
    r = first
    while r < first + n:
        d, o = divmod(r, rows)
        k = min(rows - o, first + n - r)
        acc[p, d, base + o:base + o + k, c0:c0 + val.shape[1]] += val[r - first:r - first + k, :]
        r += k


def gram_add(acc, p, x):
    add_rows(acc, p, 0, AR, 0, 0, tn(x[:, 0:B], x))
    add_rows(acc, p, 0, AR, B, 0, tn(x[:, B:2 * B], x[:, B:]))
    add_rows(acc, p, 0, AR, B, 2 * B, tn(x[:, 2 * B:], x[:, 2 * B:]))


def split3(x):
    hi = x.astype(jnp.bfloat16)
    r = x - hi.astype(jnp.float32)
    mid = r.astype(jnp.bfloat16)
    lo = (r - mid.astype(jnp.float32)).astype(jnp.bfloat16)
    return hi, mid, lo


def step_kernel(tile, inv_total, tok, dout, w_ref, ainv, y_hbm, a_out, g_out,
                buf, hbuf, ybuf, wh, acc, r1, r2a, r2b, r3a, r3b, own, ainv_v,
                ssem, rsem, lsem, tsem, ysem, asem):
    w = pl.program_id(0)
    t = pl.program_id(1)
    node = lax.axis_index('node')
    data = lax.axis_index('data')
    cy, cx, cc = node, data // 2, lax.rem(data, 2)
    partner = (cy, cx * 2 + 1 - cc)
    xn = (cy, (1 - cx) * 2 + cc)
    yn = (1 - cy, cx * 2 + cc)
    me = cy * 4 + cx * 2 + cc

    def chunk(yy, xx, c):
        return yy * 4 + xx * 2 + c

    @pl.when((w == 0) & (t == 0))
    def _():
        bar = pltpu.get_barrier_semaphore()
        for dev in (partner, xn, yn):
            pl.semaphore_signal(bar, inc=1, device_id=dev, device_id_type=MESH)
        pl.semaphore_wait(bar, 3)
        for i in range(NT):
            pltpu.make_async_copy(tok.at[pl.ds(i * tile, tile), :], buf.at[0, i], tsem.at[i]).start()

    def rcopy(src, dst, p, k, dev):
        return pltpu.make_async_remote_copy(src_ref=src, dst_ref=dst, send_sem=ssem.at[p, k], recv_sem=rsem.at[p, k],
                                            device_id=dev, device_id_type=MESH)

    def stages(rows, out, idx1, idx2, p1, p2, bwd):
        hh = rows // 2

        def c1(p):
            return [rcopy(acc.at[p, chunk(i // 2, i % 2, 1 - cc), pl.ds(0, rows)], r1.at[p, i, pl.ds(0, rows)], p, i, partner)
                    for i in range(4)]

        def c2(p):
            a = [rcopy(acc.at[p, chunk(i, 1 - cx, cc), pl.ds(0, hh)], r2a.at[p, i, pl.ds(0, hh)], p, 4 + i, xn) for i in range(2)]
            b = [rcopy(acc.at[p, chunk(1 - cy, i, cc), pl.ds(hh, hh)], r2b.at[p, i, pl.ds(0, hh)], p, 6 + i, yn) for i in range(2)]
            return a + b

        def c3(p):
            return [rcopy(acc.at[p, chunk(1 - cy, cx, cc), pl.ds(0, hh)], r3a.at[p, pl.ds(0, hh)], p, 8, yn),
                    rcopy(acc.at[p, chunk(cy, 1 - cx, cc), pl.ds(hh, hh)], r3b.at[p, pl.ds(0, hh)], p, 9, xn)]

        def c4(p, idx):
            return [rcopy(own.at[p, pl.ds(0, hh)], out.at[idx, me, pl.ds(0, hh)], p, 10, yn),
                    rcopy(own.at[p, pl.ds(hh, hh)], out.at[idx, me, pl.ds(hh, hh)], p, 11, xn)]

        def keep(p, idx):
            return pltpu.make_async_copy(own.at[p, pl.ds(0, rows)], out.at[idx, me], lsem.at[p])

        def c5(p, idx):
            def mv(d, o, k, dev):
                ref = out.at[idx, d, pl.ds(o, hh)]
                return rcopy(ref, ref, p, k, dev)
            a = [mv(chunk(i, cx, cc), 0, 12 + i, xn) for i in range(2)]
            b = [mv(chunk(cy, i, cc), hh, 14 + i, yn) for i in range(2)]
            return a + b

        def c6(p, idx):
            refs = [out.at[idx, chunk(i // 2, i % 2, cc)] for i in range(4)]
            return [rcopy(refs[i], refs[i], p, 16 + i, partner) for i in range(4)]

        def start(cs):
            for c in cs:
                c.start()

        def wait(cs):
            for c in cs:
                c.wait()

        def reduce1():
            start(c1(p1))

        def reduce2():
            wait(c1(p1))
            for i in range(4):
                acc[p1, chunk(i // 2, i % 2, cc), 0:rows, :] += r1[p1, i, 0:rows, :]
            start(c2(p1))

        def reduce3():
            wait(c2(p1))
            for i in range(2):
                acc[p1, chunk(i, cx, cc), 0:hh, :] += r2a[p1, i, 0:hh, :]
                acc[p1, chunk(cy, i, cc), hh:rows, :] += r2b[p1, i, 0:hh, :]
            start(c3(p1))

        def reduce4():
            wait(c3(p1))
            own[p1, 0:hh, :] = (acc[p1, me, 0:hh, :] + r3a[p1, 0:hh, :]) * inv_total
            own[p1, hh:rows, :] = (acc[p1, me, hh:rows, :] + r3b[p1, 0:hh, :]) * inv_total
            if bwd:
                pltpu.make_async_copy(ainv.at[L - 1 - idx1], ainv_v, asem).wait()
                gh, gm, gl = split3(own[p1, AR:SR, :])
                g3 = jnp.concatenate([gh, gm, gl], 0)
                g2 = jnp.concatenate([gh, gm], 0)
                for n in range(0, D, B):
                    ah, am, al = split3(ainv_v[n:n + B, :])
                    d1 = nt(g3, ah)
                    d2 = nt(g2, am)
                    d3 = nt(gh, al)
                    low = (d3 + d2[GR:, :]) + d1[2 * GR:, :]
                    own[p1, AR:SR, n:n + B] = (low + (d2[0:GR, :] + d1[GR:2 * GR, :])) + d1[0:GR, :]
            keep(p1, idx1).start()
            start(c4(p1, idx1))

        def gather5():
            keep(p2, idx2).wait()
            wait(c4(p2, idx2))
            start(c5(p2, idx2))

        def gather6():
            wait(c5(p2, idx2))
            start(c6(p2, idx2))

        def gather7():
            wait(c6(p2, idx2))

        return reduce1, reduce2, reduce3, reduce4, gather5, gather6, gather7

    def at(cond, step, fn):
        pl.when(cond & (t == step))(fn)

    j1, j2 = w - 1, w - 2
    p1, p2 = lax.rem(w + 1, 2), lax.rem(w, 2)
    fw = stages(AR, a_out, j1, j2, p1, p2, False)
    bw = stages(SR, g_out, j1 - L, j2 - L, p1, p2, True)
    red_f = (j1 >= 0) & (j1 < L)
    red_b = (j1 >= L) & (j1 < 2 * L)
    gat_f = (j2 >= 0) & (j2 < L)
    gat_b = (j2 >= L) & (j2 < 2 * L)

    @pl.when(red_b & (t == 0))
    def _():
        pltpu.make_async_copy(ainv.at[L - 1 - (j1 - L)], ainv_v, asem).start()

    for k, (step, rf, rb) in enumerate(((T1, red_f, red_b), (T2, red_f, red_b), (T3, red_f, red_b), (T4, red_f, red_b),
                                        (T5, gat_f, gat_b), (T6, gat_f, gat_b), (T7, gat_f, gat_b))):
        at(rf, step, fw[k])
        at(rb, step, bw[k])

    p = lax.rem(w, 2)
    slot = lax.rem(t, 2)
    half = tile // 2

    @pl.when((t == 0) & (w < 2 * L))
    def _():
        acc[p] = jnp.zeros(acc.shape[1:], jnp.float32)
        wh[...] = w_ref[0] * jnp.bfloat16(0.5)

    @pl.when(w == 0)
    def _():
        pltpu.make_async_copy(tok.at[pl.ds(t * tile, tile), :], buf.at[0, t], tsem.at[t]).wait()

    def put_y(layer, i, s):
        return pltpu.make_async_copy(ybuf.at[s], y_hbm.at[layer, pl.ds(i * tile, tile), :], ysem.at[s])

    def get_y(layer, i, s):
        return pltpu.make_async_copy(y_hbm.at[layer, pl.ds(i * tile, tile), :], ybuf.at[s], ysem.at[s])

    def get_tok(i, s):
        return pltpu.make_async_copy(tok.at[pl.ds(i * tile, tile), :], ybuf.at[s], ysem.at[s])

    @pl.when((w < L) & (w * NT + t >= 2) & (w * NT + t < (L - 1) * NT + 2))
    def _():
        put_y(0, 0, slot).wait()

    @pl.when(w < L - 1)
    def _():
        x = buf.at[p, t]
        for r in range(0, tile, half):
            for c in range(0, D, B):
                y = jnp.dot(x[r:r + half, :], wh[:, c:c + B], preferred_element_type=jnp.float32).astype(jnp.bfloat16)
                ybuf[slot, r:r + half, c:c + B] = y
                buf[1 - p, t, r:r + half, c:c + B] = gelu_value(y)
        gram_add(acc, p, x[...])
        put_y(w, t, slot).start()

    @pl.when(w == L - 1)
    def _():
        @pl.when(t == 0)
        def _():
            for i in range(NT):
                pltpu.make_async_copy(dout.at[pl.ds(i * tile, tile), :], buf.at[0, i], tsem.at[i]).start()
        gram_add(acc, p, buf[p, t])

        @pl.when(t == NT - 1)
        def _():
            get_y(L - 2, 0, 0).start()

    @pl.when(w == L)
    def _():
        pltpu.make_async_copy(dout.at[pl.ds(t * tile, tile), :], buf.at[0, t], tsem.at[t]).wait()

    wn = jnp.where(t == NT - 1, w + 1, w)
    tn_ = jnp.where(t == NT - 1, 0, t + 1)

    @pl.when((w >= L) & (wn < 2 * L - 1))
    def _():
        get_y(2 * L - 2 - wn, tn_, 1 - slot).start()

    @pl.when((w >= L) & (wn == 2 * L - 1))
    def _():
        get_tok(tn_, 1 - slot).start()

    @pl.when((w >= L) & (w < 2 * L))
    def _():
        get_tok(0, slot).wait()

    def grad_add(g, h):
        for m in range(0, D, B):
            add_rows(acc, p, AR, GR, m, 0, tn(g[:, m:m + B], h))

    @pl.when((w >= L) & (w < 2 * L - 1))
    def _():
        g = buf.at[p, t]
        for r in range(0, tile, half):
            for c in range(0, D, B):
                dh = nt(g[r:r + half, :], wh[c:c + B, :]).astype(jnp.bfloat16)
                h, slope2 = gelu_both(ybuf[slot, r:r + half, c:c + B])
                hbuf[r:r + half, c:c + B] = h
                buf[1 - p, t, r:r + half, c:c + B] = (dh.astype(jnp.float32) * slope2).astype(jnp.bfloat16)
        gram_add(acc, p, g[...])
        grad_add(g[...], hbuf[...])

    @pl.when(w == 2 * L - 1)
    def _():
        g = buf[p, t]
        gram_add(acc, p, g)
        grad_add(g, ybuf[slot])


def run_stack(tok, dout, w, a_inv, inv_total):
    n, d = tok.shape
    tile = n // NT
    f32, bf16 = jnp.float32, jnp.bfloat16
    any_spec = pl.BlockSpec(memory_space=pl.ANY)

    def w_map(i, t):
        return (jnp.where(i < L, i, jnp.clip(2 * L - 1 - i, 1, L - 1)), 0, 0)

    return pl.pallas_call(
        functools.partial(step_kernel, tile, inv_total),
        grid=(2 * L + 2, NT),
        in_specs=[any_spec, any_spec, pl.BlockSpec((1, d, d), w_map), any_spec],
        out_specs=[any_spec] * 3,
        out_shape=[
            jax.ShapeDtypeStruct((L - 1, n, d), bf16),
            jax.ShapeDtypeStruct((L, DEV, AR, d), f32),
            jax.ShapeDtypeStruct((L, DEV, SR, d), f32),
        ],
        scratch_shapes=[
            pltpu.VMEM((2, NT, tile, d), bf16),
            pltpu.VMEM((tile, d), bf16),
            pltpu.VMEM((2, tile, d), bf16),
            pltpu.VMEM((d, d), bf16),
            pltpu.VMEM((2, DEV, SR, d), f32),
            pltpu.VMEM((2, 4, SR, d), f32),
            pltpu.VMEM((2, 2, SR // 2, d), f32),
            pltpu.VMEM((2, 2, SR // 2, d), f32),
            pltpu.VMEM((2, SR // 2, d), f32),
            pltpu.VMEM((2, SR // 2, d), f32),
            pltpu.VMEM((2, SR, d), f32),
            pltpu.VMEM((d, d), f32),
            pltpu.SemaphoreType.DMA((2, 20)),
            pltpu.SemaphoreType.DMA((2, 20)),
            pltpu.SemaphoreType.DMA((2,)),
            pltpu.SemaphoreType.DMA((NT,)),
            pltpu.SemaphoreType.DMA((2,)),
            pltpu.SemaphoreType.DMA,
        ],
        compiler_params=pltpu.CompilerParams(vmem_limit_bytes=67043328, collective_id=0, has_side_effects=True),
        cost_estimate=pl.CostEstimate(flops=2 * 33 * n * d * d, bytes_accessed=200 * 2 ** 20, transcendentals=0),
        name="kfac_stack",
    )(tok, dout, w, a_inv)


def finish_kernel(a_ref, g_ref, a_old, s_old, s_inv, upd, a_new, s_new):
    def unfold(p, old, new):
        sc = (1.0 - FACTOR_DECAY)

        def put(r, c, val):
            new[0, r * B:(r + 1) * B, c * B:(c + 1) * B] = FACTOR_DECAY * old[0, r * B:(r + 1) * B, c * B:(c + 1) * B] + sc * val

        for (pr, pc, r, c) in ((0, 0, 0, 0), (0, 1, 0, 1), (0, 2, 0, 2), (1, 0, 1, 1), (1, 1, 1, 2), (1, 2, 2, 2)):
            blk = jnp.concatenate([p[0, d, 0:AR, pc * B:(pc + 1) * B] for d in range(pr * 4, pr * 4 + 4)], 0)
            put(r, c, blk)
            if r != c:
                put(c, r, blk.T)

    unfold(a_ref, a_old, a_new)
    unfold(g_ref, s_old, s_new)
    sh, sm, sl = split3(s_inv[0])
    lt = jnp.concatenate([g_ref[0, d, AR:SR, :] for d in range(DEV)], 0)
    lh, lm, ll = split3(lt)
    for m in range(0, D, B):
        x, y, z = lh[:, m:m + B], lm[:, m:m + B], ll[:, m:m + B]
        low = (tn(y, sm) + tn(x, sl)) + tn(z, sh)
        upd[0, m:m + B, :] = (low + (tn(x, sm) + tn(y, sh))) + tn(x, sh)


def finish(a_red, g_red, a_old, s_old, s_inv):
    f32 = jnp.float32
    full = pl.BlockSpec((1, D, D), lambda l: (l, 0, 0))
    shape = jax.ShapeDtypeStruct((L, D, D), f32)
    return pl.pallas_call(
        finish_kernel,
        grid=(L,),
        in_specs=[
            pl.BlockSpec((1, DEV, AR, D), lambda l: (l, 0, 0, 0)),
            pl.BlockSpec((1, DEV, SR, D), lambda l: (L - 1 - l, 0, 0, 0)),
            full, full, full,
        ],
        out_specs=[full] * 3,
        out_shape=[shape] * 3,
        compiler_params=pltpu.CompilerParams(vmem_limit_bytes=60 * 2 ** 20),
        cost_estimate=pl.CostEstimate(flops=L * 12 * D ** 3, bytes_accessed=160 * 2 ** 20, transcendentals=0),
        name="kfac_finish",
    )(a_red, g_red, a_old, s_old, s_inv)


def solution(mesh):
    batch_axes = ('node', 'data')
    row_spec = P(batch_axes, None)
    full_spec = P()

    def kfac_step(tokens, grad_out, weights, a_old, s_old, a_inv, s_inv):
        inv_total = 1.0 / tokens.shape[0]

        def per_device(tok, dout, w, a_prev, s_prev, a_pre, s_pre):
            _, a_red, g_red = run_stack(tok, dout, w, a_pre, inv_total)
            return tuple(finish(a_red, g_red, a_prev, s_prev, s_pre))

        return jax.shard_map(per_device, mesh=mesh, in_specs=(row_spec, row_spec, full_spec, full_spec, full_spec, full_spec, full_spec), out_specs=(full_spec, full_spec, full_spec), check_vma=False)(tokens, grad_out, weights, a_old, s_old, a_inv, s_inv)

    return kfac_step
```

```python
import functools
import jax
import jax.numpy as jnp
from jax import lax
from jax.experimental import pallas as pl
from jax.experimental.pallas import tpu as pltpu
from jax.sharding import PartitionSpec as P

FACTOR_DECAY = 0.8
GELU_SCALE = 0.7978845608028654
GELU_CUBIC = 0.044715
D = 768
B = 256
NT = 8
DEV = 8
AR = 64
GR = 96
SR = AR + GR
L = 8
MESH = pl.DeviceIdType.MESH
T1, T2, T3, T4, T5, T6, T7 = 0, 1, 4, 0, 4, 0, 2


def tn(left, right):
    return lax.dot_general(left, right, (((0,), (0,)), ((), ())), preferred_element_type=jnp.float32)


def nt(left, right):
    return lax.dot_general(left, right, (((1,), (1,)), ((), ())), preferred_element_type=jnp.float32)


def half_parts(half_act):
    y = half_act.astype(jnp.float32)
    sq = jnp.minimum(y * y, 1e37)
    kp = (8.0 * GELU_SCALE * GELU_CUBIC) * sq
    a = 2.0 * GELU_SCALE + kp
    return y, kp, a, jnp.tanh(y * a)


def gelu_value(half_act):
    y, _, _, t = half_parts(half_act)
    return (y + y * t).astype(jnp.bfloat16)


def gelu_both(half_act):
    y, kp, a, t = half_parts(half_act)
    opt = 1.0 + t
    h = y * opt
    slope2 = opt + (h * (1.0 - t)) * ((a + kp) + kp)
    return h.astype(jnp.bfloat16), slope2


def add_rows(acc, p, base, rows, first, c0, val):
    n = val.shape[0]
    r = first
    while r < first + n:
        d, o = divmod(r, rows)
        k = min(rows - o, first + n - r)
        acc[p, d, base + o:base + o + k, c0:c0 + val.shape[1]] += val[r - first:r - first + k, :]
        r += k


def gram_add(acc, p, x):
    add_rows(acc, p, 0, AR, 0, 0, tn(x[:, 0:B], x))
    add_rows(acc, p, 0, AR, B, 0, tn(x[:, B:2 * B], x[:, B:]))
    add_rows(acc, p, 0, AR, B, 2 * B, tn(x[:, 2 * B:], x[:, 2 * B:]))


def split3(x):
    hi = x.astype(jnp.bfloat16)
    r = x - hi.astype(jnp.float32)
    mid = r.astype(jnp.bfloat16)
    lo = (r - mid.astype(jnp.float32)).astype(jnp.bfloat16)
    return hi, mid, lo


def step_kernel(tile, inv_total, tok, dout, w_ref, ainv, y_hbm, a_out, g_out,
                buf, obuf, hbuf, ybuf, wh, acc, r1, r2a, r2b, r3a, r3b, own, ainv_v,
                ssem, rsem, lsem, tsem, ysem, osem, asem):
    w = pl.program_id(0)
    t = pl.program_id(1)
    node = lax.axis_index('node')
    data = lax.axis_index('data')
    cy, cx, cc = node, data // 2, lax.rem(data, 2)
    partner = (cy, cx * 2 + 1 - cc)
    xn = (cy, (1 - cx) * 2 + cc)
    yn = (1 - cy, cx * 2 + cc)
    me = cy * 4 + cx * 2 + cc

    def chunk(yy, xx, c):
        return yy * 4 + xx * 2 + c

    @pl.when((w == 0) & (t == 0))
    def _():
        bar = pltpu.get_barrier_semaphore()
        for dev in (partner, xn, yn):
            pl.semaphore_signal(bar, inc=1, device_id=dev, device_id_type=MESH)
        pl.semaphore_wait(bar, 3)
        for i in range(NT):
            pltpu.make_async_copy(tok.at[pl.ds(i * tile, tile), :], buf.at[i], tsem.at[i]).start()

    def rcopy(src, dst, p, k, dev):
        return pltpu.make_async_remote_copy(src_ref=src, dst_ref=dst, send_sem=ssem.at[p, k], recv_sem=rsem.at[p, k],
                                            device_id=dev, device_id_type=MESH)

    def stages(rows, out, idx2, idx3, p1, p2, p3, bwd):
        hh = rows // 2

        def c1(p):
            return [rcopy(acc.at[p, chunk(i // 2, i % 2, 1 - cc), pl.ds(0, rows)], r1.at[p, i, pl.ds(0, rows)], p, i, partner)
                    for i in range(4)]

        def c2(p):
            a = [rcopy(acc.at[p, chunk(i, 1 - cx, cc), pl.ds(0, hh)], r2a.at[p, i, pl.ds(0, hh)], p, 4 + i, xn) for i in range(2)]
            b = [rcopy(acc.at[p, chunk(1 - cy, i, cc), pl.ds(hh, hh)], r2b.at[p, i, pl.ds(0, hh)], p, 6 + i, yn) for i in range(2)]
            return a + b

        def c3(p):
            return [rcopy(acc.at[p, chunk(1 - cy, cx, cc), pl.ds(0, hh)], r3a.at[p, pl.ds(0, hh)], p, 8, yn),
                    rcopy(acc.at[p, chunk(cy, 1 - cx, cc), pl.ds(hh, hh)], r3b.at[p, pl.ds(0, hh)], p, 9, xn)]

        def c4(p, idx):
            return [rcopy(own.at[p, pl.ds(0, hh)], out.at[idx, me, pl.ds(0, hh)], p, 10, yn),
                    rcopy(own.at[p, pl.ds(hh, hh)], out.at[idx, me, pl.ds(hh, hh)], p, 11, xn)]

        def keep(p, idx):
            return pltpu.make_async_copy(own.at[p, pl.ds(0, rows)], out.at[idx, me], lsem.at[p])

        def c5(p, idx):
            def mv(d, o, k, dev):
                ref = out.at[idx, d, pl.ds(o, hh)]
                return rcopy(ref, ref, p, k, dev)
            a = [mv(chunk(i, cx, cc), 0, 12 + i, xn) for i in range(2)]
            b = [mv(chunk(cy, i, cc), hh, 14 + i, yn) for i in range(2)]
            return a + b

        def c6(p, idx):
            refs = [out.at[idx, chunk(i // 2, i % 2, cc)] for i in range(4)]
            return [rcopy(refs[i], refs[i], p, 16 + i, partner) for i in range(4)]

        def start(cs):
            for c in cs:
                c.start()

        def wait(cs):
            for c in cs:
                c.wait()

        def reduce1():
            start(c1(p1))

        def reduce2():
            wait(c1(p1))
            for i in range(4):
                acc[p1, chunk(i // 2, i % 2, cc), 0:rows, :] += r1[p1, i, 0:rows, :]
            start(c2(p1))

        def reduce3():
            wait(c2(p1))
            for i in range(2):
                acc[p1, chunk(i, cx, cc), 0:hh, :] += r2a[p1, i, 0:hh, :]
                acc[p1, chunk(cy, i, cc), hh:rows, :] += r2b[p1, i, 0:hh, :]
            start(c3(p1))

        def reduce4():
            wait(c3(p2))
            own[p2, 0:hh, :] = (acc[p2, me, 0:hh, :] + r3a[p2, 0:hh, :]) * inv_total
            own[p2, hh:rows, :] = (acc[p2, me, hh:rows, :] + r3b[p2, 0:hh, :]) * inv_total
            if bwd:
                pltpu.make_async_copy(ainv.at[L - 1 - idx2], ainv_v, asem).wait()
                gh, gm, gl = split3(own[p2, AR:SR, :])
                g3 = jnp.concatenate([gh, gm, gl], 0)
                g2 = jnp.concatenate([gh, gm], 0)
                for n in range(0, D, B):
                    ah, am, al = split3(ainv_v[n:n + B, :])
                    d1 = nt(g3, ah)
                    d2 = nt(g2, am)
                    d3 = nt(gh, al)
                    low = (d3 + d2[GR:, :]) + d1[2 * GR:, :]
                    own[p2, AR:SR, n:n + B] = (low + (d2[0:GR, :] + d1[GR:2 * GR, :])) + d1[0:GR, :]
            keep(p2, idx2).start()
            start(c4(p2, idx2))

        def gather5():
            keep(p2, idx2).wait()
            wait(c4(p2, idx2))
            start(c5(p2, idx2))

        def gather6():
            wait(c5(p3, idx3))
            start(c6(p3, idx3))

        def gather7():
            wait(c6(p3, idx3))

        return reduce1, reduce2, reduce3, reduce4, gather5, gather6, gather7

    def at(cond, step, fn):
        pl.when(cond & (t == step))(fn)

    j1, j2, j3 = w - 1, w - 2, w - 3
    p1, p2, p3 = lax.rem(w + 1, 2), lax.rem(w, 2), lax.rem(w + 1, 2)
    fw = stages(AR, a_out, j2, j3, p1, p2, p3, False)
    bw = stages(SR, g_out, j2 - L, j3 - L, p1, p2, p3, True)
    is_f = [(j >= 0) & (j < L) for j in (j1, j2, j3)]
    is_b = [(j >= L) & (j < 2 * L) for j in (j1, j2, j3)]

    for k, (step, i) in enumerate(((T1, 0), (T2, 0), (T3, 0), (T4, 1), (T5, 1), (T6, 2), (T7, 2))):
        at(is_f[i], step, fw[k])
        at(is_b[i], step, bw[k])

    @pl.when(is_b[0] & (t == 4))
    def _():
        pltpu.make_async_copy(ainv.at[L - 1 - (j1 - L)], ainv_v, asem).start()

    p = lax.rem(w, 2)
    slot = lax.rem(t, 2)
    rs = min(tile, B)

    @pl.when((t == 0) & (w < 2 * L))
    def _():
        acc[p] = jnp.zeros(acc.shape[1:], jnp.float32)
        wh[...] = w_ref[0] * jnp.bfloat16(0.5)

    @pl.when(w == 0)
    def _():
        pltpu.make_async_copy(tok.at[pl.ds(t * tile, tile), :], buf.at[t], tsem.at[t]).wait()

    def put_y(layer, i, s):
        return pltpu.make_async_copy(ybuf.at[s], y_hbm.at[layer, pl.ds(i * tile, tile), :], ysem.at[s])

    def get_y(layer, i, s):
        return pltpu.make_async_copy(y_hbm.at[layer, pl.ds(i * tile, tile), :], ybuf.at[s], ysem.at[s])

    def get_tok(i, s):
        return pltpu.make_async_copy(tok.at[pl.ds(i * tile, tile), :], ybuf.at[s], ysem.at[s])

    def put_o(i, s):
        return pltpu.make_async_copy(obuf.at[s], buf.at[i], osem.at[s])

    g_step = w * NT + t
    fwd_out = (g_step >= 2) & (g_step < (L - 1) * NT + 2)

    @pl.when(fwd_out)
    def _():
        put_y(0, 0, slot).wait()

    @pl.when(fwd_out | ((g_step >= L * NT + 2) & (g_step < (2 * L - 1) * NT + 2)))
    def _():
        put_o(0, slot).wait()

    @pl.when(w < L - 1)
    def _():
        x = buf.at[t]
        for r in range(0, tile, rs):
            for c in range(0, D, B):
                y = jnp.dot(x[r:r + rs, :], wh[:, c:c + B], preferred_element_type=jnp.float32).astype(jnp.bfloat16)
                ybuf[slot, r:r + rs, c:c + B] = y
                obuf[slot, r:r + rs, c:c + B] = gelu_value(y)
        gram_add(acc, p, x[...])
        put_y(w, t, slot).start()
        put_o(t, slot).start()

    @pl.when(w == L - 1)
    def _():
        gram_add(acc, p, buf[t])
        pltpu.make_async_copy(dout.at[pl.ds(t * tile, tile), :], buf.at[t], tsem.at[t]).start()

        @pl.when(t == NT - 1)
        def _():
            get_y(L - 2, 0, 0).start()

    @pl.when(w == L)
    def _():
        pltpu.make_async_copy(dout.at[pl.ds(t * tile, tile), :], buf.at[t], tsem.at[t]).wait()

    wn = jnp.where(t == NT - 1, w + 1, w)
    tn_ = jnp.where(t == NT - 1, 0, t + 1)

    @pl.when((w >= L) & (wn < 2 * L - 1))
    def _():
        get_y(2 * L - 2 - wn, tn_, 1 - slot).start()

    @pl.when((w >= L) & (wn == 2 * L - 1))
    def _():
        get_tok(tn_, 1 - slot).start()

    @pl.when((w >= L) & (w < 2 * L))
    def _():
        get_tok(0, slot).wait()

    def grad_add(g, h):
        for m in range(0, D, B):
            add_rows(acc, p, AR, GR, m, 0, tn(g[:, m:m + B], h))

    @pl.when((w >= L) & (w < 2 * L - 1))
    def _():
        g = buf.at[t]
        for r in range(0, tile, rs):
            for c in range(0, D, B):
                dh = nt(g[r:r + rs, :], wh[c:c + B, :]).astype(jnp.bfloat16)
                h, slope2 = gelu_both(ybuf[slot, r:r + rs, c:c + B])
                hbuf[r:r + rs, c:c + B] = h
                obuf[slot, r:r + rs, c:c + B] = (dh.astype(jnp.float32) * slope2).astype(jnp.bfloat16)
        gram_add(acc, p, g[...])
        grad_add(g[...], hbuf[...])
        put_o(t, slot).start()

    @pl.when(w == 2 * L - 1)
    def _():
        g = buf[t]
        gram_add(acc, p, g)
        grad_add(g, ybuf[slot])


def run_stack(tok, dout, w, a_inv, inv_total):
    n, d = tok.shape
    tile = n // NT
    f32, bf16 = jnp.float32, jnp.bfloat16
    any_spec = pl.BlockSpec(memory_space=pl.ANY)

    def w_map(i, t):
        return (jnp.where(i < L, i, jnp.clip(2 * L - 1 - i, 1, L - 1)), 0, 0)

    return pl.pallas_call(
        functools.partial(step_kernel, tile, inv_total),
        grid=(2 * L + 3, NT),
        in_specs=[any_spec, any_spec, pl.BlockSpec((1, d, d), w_map), any_spec],
        out_specs=[any_spec] * 3,
        out_shape=[
            jax.ShapeDtypeStruct((L - 1, n, d), bf16),
            jax.ShapeDtypeStruct((L, DEV, AR, d), f32),
            jax.ShapeDtypeStruct((L, DEV, SR, d), f32),
        ],
        scratch_shapes=[
            pltpu.VMEM((NT, tile, d), bf16),
            pltpu.VMEM((2, tile, d), bf16),
            pltpu.VMEM((tile, d), bf16),
            pltpu.VMEM((2, tile, d), bf16),
            pltpu.VMEM((d, d), bf16),
            pltpu.VMEM((2, DEV, SR, d), f32),
            pltpu.VMEM((2, 4, SR, d), f32),
            pltpu.VMEM((2, 2, SR // 2, d), f32),
            pltpu.VMEM((2, 2, SR // 2, d), f32),
            pltpu.VMEM((2, SR // 2, d), f32),
            pltpu.VMEM((2, SR // 2, d), f32),
            pltpu.VMEM((2, SR, d), f32),
            pltpu.VMEM((d, d), f32),
            pltpu.SemaphoreType.DMA((2, 20)),
            pltpu.SemaphoreType.DMA((2, 20)),
            pltpu.SemaphoreType.DMA((2,)),
            pltpu.SemaphoreType.DMA((NT,)),
            pltpu.SemaphoreType.DMA((2,)),
            pltpu.SemaphoreType.DMA((2,)),
            pltpu.SemaphoreType.DMA,
        ],
        compiler_params=pltpu.CompilerParams(vmem_limit_bytes=67043328, collective_id=0, has_side_effects=True),
        cost_estimate=pl.CostEstimate(flops=2 * 33 * n * d * d, bytes_accessed=200 * 2 ** 20, transcendentals=0),
        name="kfac_stack",
    )(tok, dout, w, a_inv)


def finish_kernel(a_ref, g_ref, a_old, s_old, s_inv, upd, a_new, s_new):
    def unfold(p, old, new):
        sc = (1.0 - FACTOR_DECAY)

        def put(r, c, val):
            new[0, r * B:(r + 1) * B, c * B:(c + 1) * B] = FACTOR_DECAY * old[0, r * B:(r + 1) * B, c * B:(c + 1) * B] + sc * val

        for (pr, pc, r, c) in ((0, 0, 0, 0), (0, 1, 0, 1), (0, 2, 0, 2), (1, 0, 1, 1), (1, 1, 1, 2), (1, 2, 2, 2)):
            blk = jnp.concatenate([p[0, d, 0:AR, pc * B:(pc + 1) * B] for d in range(pr * 4, pr * 4 + 4)], 0)
            put(r, c, blk)
            if r != c:
                put(c, r, blk.T)

    unfold(a_ref, a_old, a_new)
    unfold(g_ref, s_old, s_new)
    sh, sm, sl = split3(s_inv[0])
    lt = jnp.concatenate([g_ref[0, d, AR:SR, :] for d in range(DEV)], 0)
    lh, lm, ll = split3(lt)
    for m in range(0, D, B):
        x, y, z = lh[:, m:m + B], lm[:, m:m + B], ll[:, m:m + B]
        low = (tn(y, sm) + tn(x, sl)) + tn(z, sh)
        upd[0, m:m + B, :] = (low + (tn(x, sm) + tn(y, sh))) + tn(x, sh)


def finish(a_red, g_red, a_old, s_old, s_inv):
    f32 = jnp.float32
    full = pl.BlockSpec((1, D, D), lambda l: (l, 0, 0))
    shape = jax.ShapeDtypeStruct((L, D, D), f32)
    return pl.pallas_call(
        finish_kernel,
        grid=(L,),
        in_specs=[
            pl.BlockSpec((1, DEV, AR, D), lambda l: (l, 0, 0, 0)),
            pl.BlockSpec((1, DEV, SR, D), lambda l: (L - 1 - l, 0, 0, 0)),
            full, full, full,
        ],
        out_specs=[full] * 3,
        out_shape=[shape] * 3,
        compiler_params=pltpu.CompilerParams(vmem_limit_bytes=60 * 2 ** 20),
        cost_estimate=pl.CostEstimate(flops=L * 12 * D ** 3, bytes_accessed=160 * 2 ** 20, transcendentals=0),
        name="kfac_finish",
    )(a_red, g_red, a_old, s_old, s_inv)


def solution(mesh):
    batch_axes = ('node', 'data')
    row_spec = P(batch_axes, None)
    full_spec = P()

    def kfac_step(tokens, grad_out, weights, a_old, s_old, a_inv, s_inv):
        inv_total = 1.0 / tokens.shape[0]

        def per_device(tok, dout, w, a_prev, s_prev, a_pre, s_pre):
            _, a_red, g_red = run_stack(tok, dout, w, a_pre, inv_total)
            return tuple(finish(a_red, g_red, a_prev, s_prev, s_pre))

        return jax.shard_map(per_device, mesh=mesh, in_specs=(row_spec, row_spec, full_spec, full_spec, full_spec, full_spec, full_spec), out_specs=(full_spec, full_spec, full_spec), check_vma=False)(tokens, grad_out, weights, a_old, s_old, a_inv, s_inv)

    return kfac_step
```

```python
import functools
import jax
import jax.numpy as jnp
from jax import lax
from jax.experimental import pallas as pl
from jax.experimental.pallas import tpu as pltpu
from jax.sharding import PartitionSpec as P

FACTOR_DECAY = 0.8
GELU_SCALE = 0.7978845608028654
GELU_CUBIC = 0.044715
D = 768
B = 256
NT = 8
DEV = 8
AR = 64
GR = 96
SR = AR + GR
L = 8
MESH = pl.DeviceIdType.MESH
T1, T2, T3, T4, T5, T6, T7 = 0, 1, 0, 4, 2, 2, 4


def tn(left, right):
    return lax.dot_general(left, right, (((0,), (0,)), ((), ())), preferred_element_type=jnp.float32)


def nt(left, right):
    return lax.dot_general(left, right, (((1,), (1,)), ((), ())), preferred_element_type=jnp.float32)


def half_parts(half_act):
    y = half_act.astype(jnp.float32)
    sq = jnp.minimum(y * y, 1e37)
    kp = (8.0 * GELU_SCALE * GELU_CUBIC) * sq
    a = 2.0 * GELU_SCALE + kp
    return y, kp, a, jnp.tanh(y * a)


def gelu_value(half_act):
    y, _, _, t = half_parts(half_act)
    return (y + y * t).astype(jnp.bfloat16)


def gelu_both(half_act):
    y, kp, a, t = half_parts(half_act)
    opt = 1.0 + t
    h = y * opt
    slope2 = opt + (h * (1.0 - t)) * ((a + kp) + kp)
    return h.astype(jnp.bfloat16), slope2


def add_rows(acc, p, base, rows, first, c0, val):
    n = val.shape[0]
    r = first
    while r < first + n:
        d, o = divmod(r, rows)
        k = min(rows - o, first + n - r)
        acc[p, d, base + o:base + o + k, c0:c0 + val.shape[1]] += val[r - first:r - first + k, :]
        r += k


def gram_add(acc, p, x):
    add_rows(acc, p, 0, AR, 0, 0, tn(x[:, 0:B], x))
    add_rows(acc, p, 0, AR, B, 0, tn(x[:, B:2 * B], x[:, B:]))
    add_rows(acc, p, 0, AR, B, 2 * B, tn(x[:, 2 * B:], x[:, 2 * B:]))


def split3(x):
    hi = x.astype(jnp.bfloat16)
    r = x - hi.astype(jnp.float32)
    mid = r.astype(jnp.bfloat16)
    lo = (r - mid.astype(jnp.float32)).astype(jnp.bfloat16)
    return hi, mid, lo


def step_kernel(tile, inv_total, tok, dout, w_ref, ainv, y_hbm, a_out, g_out,
                buf, obuf, hbuf, ybuf, wh, acc, r1, r2a, r2b, r3a, r3b, own, ainv_v,
                ssem, rsem, lsem, tsem, ysem, osem, asem):
    w = pl.program_id(0)
    t = pl.program_id(1)
    node = lax.axis_index('node')
    data = lax.axis_index('data')
    cy, cx, cc = node, data // 2, lax.rem(data, 2)
    partner = (cy, cx * 2 + 1 - cc)
    xn = (cy, (1 - cx) * 2 + cc)
    yn = (1 - cy, cx * 2 + cc)
    me = cy * 4 + cx * 2 + cc

    def chunk(yy, xx, c):
        return yy * 4 + xx * 2 + c

    @pl.when((w == 0) & (t == 0))
    def _():
        bar = pltpu.get_barrier_semaphore()
        for dev in (partner, xn, yn):
            pl.semaphore_signal(bar, inc=1, device_id=dev, device_id_type=MESH)
        pl.semaphore_wait(bar, 3)
        for i in range(NT):
            pltpu.make_async_copy(tok.at[pl.ds(i * tile, tile), :], buf.at[i], tsem.at[i]).start()

    def rcopy(src, dst, p, k, dev):
        return pltpu.make_async_remote_copy(src_ref=src, dst_ref=dst, send_sem=ssem.at[p, k], recv_sem=rsem.at[p, k],
                                            device_id=dev, device_id_type=MESH)

    def stages(rows, out, idx2, idx3, idx4, bwd):
        hh = rows // 2

        def c1(p, q):
            return [rcopy(acc.at[q, chunk(i // 2, i % 2, 1 - cc), pl.ds(0, rows)], r1.at[p, i, pl.ds(0, rows)], p, i, partner)
                    for i in range(4)]

        def c2(p, q):
            a = [rcopy(acc.at[q, chunk(i, 1 - cx, cc), pl.ds(0, hh)], r2a.at[p, i, pl.ds(0, hh)], p, 4 + i, xn) for i in range(2)]
            b = [rcopy(acc.at[q, chunk(1 - cy, i, cc), pl.ds(hh, hh)], r2b.at[p, i, pl.ds(0, hh)], p, 6 + i, yn) for i in range(2)]
            return a + b

        def c3(p, q):
            return [rcopy(acc.at[q, chunk(1 - cy, cx, cc), pl.ds(0, hh)], r3a.at[p, pl.ds(0, hh)], p, 8, yn),
                    rcopy(acc.at[q, chunk(cy, 1 - cx, cc), pl.ds(hh, hh)], r3b.at[p, pl.ds(0, hh)], p, 9, xn)]

        def c4(p, idx):
            return [rcopy(own.at[p, pl.ds(0, hh)], out.at[idx, me, pl.ds(0, hh)], p, 10, yn),
                    rcopy(own.at[p, pl.ds(hh, hh)], out.at[idx, me, pl.ds(hh, hh)], p, 11, xn)]

        def keep(p, idx):
            return pltpu.make_async_copy(own.at[p, pl.ds(0, rows)], out.at[idx, me], lsem.at[p])

        def c5(p, idx):
            def mv(d, o, k, dev):
                ref = out.at[idx, d, pl.ds(o, hh)]
                return rcopy(ref, ref, p, k, dev)
            a = [mv(chunk(i, cx, cc), 0, 12 + i, xn) for i in range(2)]
            b = [mv(chunk(cy, i, cc), hh, 14 + i, yn) for i in range(2)]
            return a + b

        def c6(p, idx):
            refs = [out.at[idx, chunk(i // 2, i % 2, cc)] for i in range(4)]
            return [rcopy(refs[i], refs[i], p, 16 + i, partner) for i in range(4)]

        def start(cs):
            for c in cs:
                c.start()

        def wait(cs):
            for c in cs:
                c.wait()

        def reduce1():
            start(c1(p1, q1))

        def reduce2():
            wait(c1(p1, q1))
            for i in range(4):
                acc[q1, chunk(i // 2, i % 2, cc), 0:rows, :] += r1[p1, i, 0:rows, :]
            start(c2(p1, q1))

        def reduce3():
            wait(c2(p2, q2))
            for i in range(2):
                acc[q2, chunk(i, cx, cc), 0:hh, :] += r2a[p2, i, 0:hh, :]
                acc[q2, chunk(cy, i, cc), hh:rows, :] += r2b[p2, i, 0:hh, :]
            start(c3(p2, q2))

        def reduce4():
            wait(c3(p2, q2))
            own[p2, 0:hh, :] = (acc[q2, me, 0:hh, :] + r3a[p2, 0:hh, :]) * inv_total
            own[p2, hh:rows, :] = (acc[q2, me, hh:rows, :] + r3b[p2, 0:hh, :]) * inv_total
            if bwd:
                pltpu.make_async_copy(ainv.at[L - 1 - idx2], ainv_v, asem).wait()
                gh, gm, gl = split3(own[p2, AR:SR, :])
                g3 = jnp.concatenate([gh, gm, gl], 0)
                g2 = jnp.concatenate([gh, gm], 0)
                for n in range(0, D, B):
                    ah, am, al = split3(ainv_v[n:n + B, :])
                    d1 = nt(g3, ah)
                    d2 = nt(g2, am)
                    d3 = nt(gh, al)
                    low = (d3 + d2[GR:, :]) + d1[2 * GR:, :]
                    own[p2, AR:SR, n:n + B] = (low + (d2[0:GR, :] + d1[GR:2 * GR, :])) + d1[0:GR, :]
            keep(p2, idx2).start()
            start(c4(p2, idx2))

        def gather5():
            keep(p3, idx3).wait()
            wait(c4(p3, idx3))
            start(c5(p3, idx3))

        def gather6():
            wait(c5(p4, idx4))
            start(c6(p4, idx4))

        def gather7():
            wait(c6(p4, idx4))

        return reduce1, reduce2, reduce3, reduce4, gather5, gather6, gather7

    def at(cond, step, fn):
        pl.when(cond & (t == step))(fn)

    j1, j2, j3, j4 = w - 1, w - 2, w - 3, w - 4
    p1, p2, p3, p4 = lax.rem(w + 1, 2), lax.rem(w, 2), lax.rem(w + 1, 2), lax.rem(w, 2)
    q1, q2 = lax.rem(w + 2, 3), lax.rem(w + 1, 3)
    fw = stages(AR, a_out, j2, j3, j4, False)
    bw = stages(SR, g_out, j2 - L, j3 - L, j4 - L, True)
    is_f = [(j >= 0) & (j < L) for j in (j1, j2, j3, j4)]
    is_b = [(j >= L) & (j < 2 * L) for j in (j1, j2, j3, j4)]

    @pl.when(is_b[1] & (t == 0))
    def _():
        pltpu.make_async_copy(ainv.at[L - 1 - (j2 - L)], ainv_v, asem).start()

    for k, step, i in ((0, T1, 0), (2, T3, 1), (1, T2, 0), (5, T6, 3), (4, T5, 2), (3, T4, 1), (6, T7, 3)):
        at(is_f[i], step, fw[k])
        at(is_b[i], step, bw[k])

    p = lax.rem(w, 3)
    slot = lax.rem(t, 2)
    rs = min(tile, B)

    @pl.when((t == 0) & (w < 2 * L))
    def _():
        acc[p] = jnp.zeros(acc.shape[1:], jnp.float32)
        wh[...] = w_ref[0] * jnp.bfloat16(0.5)

    @pl.when(w == 0)
    def _():
        pltpu.make_async_copy(tok.at[pl.ds(t * tile, tile), :], buf.at[t], tsem.at[t]).wait()

    def put_y(layer, i, s):
        return pltpu.make_async_copy(ybuf.at[s], y_hbm.at[layer, pl.ds(i * tile, tile), :], ysem.at[s])

    def get_y(layer, i, s):
        return pltpu.make_async_copy(y_hbm.at[layer, pl.ds(i * tile, tile), :], ybuf.at[s], ysem.at[s])

    def get_tok(i, s):
        return pltpu.make_async_copy(tok.at[pl.ds(i * tile, tile), :], ybuf.at[s], ysem.at[s])

    def put_o(i, s):
        return pltpu.make_async_copy(obuf.at[s], buf.at[i], osem.at[s])

    g_step = w * NT + t
    fwd_out = (g_step >= 2) & (g_step < (L - 1) * NT + 2)

    @pl.when(fwd_out)
    def _():
        put_y(0, 0, slot).wait()

    @pl.when(fwd_out | ((g_step >= L * NT + 2) & (g_step < (2 * L - 1) * NT + 2)))
    def _():
        put_o(0, slot).wait()

    @pl.when(w < L - 1)
    def _():
        x = buf.at[t]
        for r in range(0, tile, rs):
            for c in range(0, D, B):
                y = jnp.dot(x[r:r + rs, :], wh[:, c:c + B], preferred_element_type=jnp.float32).astype(jnp.bfloat16)
                ybuf[slot, r:r + rs, c:c + B] = y
                obuf[slot, r:r + rs, c:c + B] = gelu_value(y)
        gram_add(acc, p, x[...])
        put_y(w, t, slot).start()
        put_o(t, slot).start()

    @pl.when(w == L - 1)
    def _():
        gram_add(acc, p, buf[t])
        pltpu.make_async_copy(dout.at[pl.ds(t * tile, tile), :], buf.at[t], tsem.at[t]).start()

        @pl.when(t == NT - 1)
        def _():
            get_y(L - 2, 0, 0).start()

    @pl.when(w == L)
    def _():
        pltpu.make_async_copy(dout.at[pl.ds(t * tile, tile), :], buf.at[t], tsem.at[t]).wait()

    wn = jnp.where(t == NT - 1, w + 1, w)
    tn_ = jnp.where(t == NT - 1, 0, t + 1)

    @pl.when((w >= L) & (wn < 2 * L - 1))
    def _():
        get_y(2 * L - 2 - wn, tn_, 1 - slot).start()

    @pl.when((w >= L) & (wn == 2 * L - 1))
    def _():
        get_tok(tn_, 1 - slot).start()

    @pl.when((w >= L) & (w < 2 * L))
    def _():
        get_tok(0, slot).wait()

    def grad_add(g, h):
        for m in range(0, D, B):
            add_rows(acc, p, AR, GR, m, 0, tn(g[:, m:m + B], h))

    @pl.when((w >= L) & (w < 2 * L - 1))
    def _():
        g = buf.at[t]
        for r in range(0, tile, rs):
            for c in range(0, D, B):
                dh = nt(g[r:r + rs, :], wh[c:c + B, :]).astype(jnp.bfloat16)
                h, slope2 = gelu_both(ybuf[slot, r:r + rs, c:c + B])
                hbuf[r:r + rs, c:c + B] = h
                obuf[slot, r:r + rs, c:c + B] = (dh.astype(jnp.float32) * slope2).astype(jnp.bfloat16)
        gram_add(acc, p, g[...])
        grad_add(g[...], hbuf[...])
        put_o(t, slot).start()

    @pl.when(w == 2 * L - 1)
    def _():
        g = buf[t]
        gram_add(acc, p, g)
        grad_add(g, ybuf[slot])


def run_stack(tok, dout, w, a_inv, inv_total):
    n, d = tok.shape
    tile = n // NT
    f32, bf16 = jnp.float32, jnp.bfloat16
    any_spec = pl.BlockSpec(memory_space=pl.ANY)

    def w_map(i, t):
        return (jnp.where(i < L, i, jnp.clip(2 * L - 1 - i, 1, L - 1)), 0, 0)

    return pl.pallas_call(
        functools.partial(step_kernel, tile, inv_total),
        grid=(2 * L + 4, NT),
        in_specs=[any_spec, any_spec, pl.BlockSpec((1, d, d), w_map), any_spec],
        out_specs=[any_spec] * 3,
        out_shape=[
            jax.ShapeDtypeStruct((L - 1, n, d), bf16),
            jax.ShapeDtypeStruct((L, DEV, AR, d), f32),
            jax.ShapeDtypeStruct((L, DEV, SR, d), f32),
        ],
        scratch_shapes=[
            pltpu.VMEM((NT, tile, d), bf16),
            pltpu.VMEM((2, tile, d), bf16),
            pltpu.VMEM((tile, d), bf16),
            pltpu.VMEM((2, tile, d), bf16),
            pltpu.VMEM((d, d), bf16),
            pltpu.VMEM((3, DEV, SR, d), f32),
            pltpu.VMEM((2, 4, SR, d), f32),
            pltpu.VMEM((2, 2, SR // 2, d), f32),
            pltpu.VMEM((2, 2, SR // 2, d), f32),
            pltpu.VMEM((2, SR // 2, d), f32),
            pltpu.VMEM((2, SR // 2, d), f32),
            pltpu.VMEM((2, SR, d), f32),
            pltpu.VMEM((d, d), f32),
            pltpu.SemaphoreType.DMA((2, 20)),
            pltpu.SemaphoreType.DMA((2, 20)),
            pltpu.SemaphoreType.DMA((2,)),
            pltpu.SemaphoreType.DMA((NT,)),
            pltpu.SemaphoreType.DMA((2,)),
            pltpu.SemaphoreType.DMA((2,)),
            pltpu.SemaphoreType.DMA,
        ],
        compiler_params=pltpu.CompilerParams(vmem_limit_bytes=67043328, collective_id=0, has_side_effects=True),
        cost_estimate=pl.CostEstimate(flops=2 * 33 * n * d * d, bytes_accessed=200 * 2 ** 20, transcendentals=0),
        name="kfac_stack",
    )(tok, dout, w, a_inv)


def finish_kernel(a_ref, g_ref, a_old, s_old, s_inv, upd, a_new, s_new):
    def unfold(p, old, new):
        sc = (1.0 - FACTOR_DECAY)

        def put(r, c, val):
            new[0, r * B:(r + 1) * B, c * B:(c + 1) * B] = FACTOR_DECAY * old[0, r * B:(r + 1) * B, c * B:(c + 1) * B] + sc * val

        for (pr, pc, r, c) in ((0, 0, 0, 0), (0, 1, 0, 1), (0, 2, 0, 2), (1, 0, 1, 1), (1, 1, 1, 2), (1, 2, 2, 2)):
            blk = jnp.concatenate([p[0, d, 0:AR, pc * B:(pc + 1) * B] for d in range(pr * 4, pr * 4 + 4)], 0)
            put(r, c, blk)
            if r != c:
                put(c, r, blk.T)

    unfold(a_ref, a_old, a_new)
    unfold(g_ref, s_old, s_new)
    sh, sm, sl = split3(s_inv[0])
    lt = jnp.concatenate([g_ref[0, d, AR:SR, :] for d in range(DEV)], 0)
    lh, lm, ll = split3(lt)
    for m in range(0, D, B):
        x, y, z = lh[:, m:m + B], lm[:, m:m + B], ll[:, m:m + B]
        low = (tn(y, sm) + tn(x, sl)) + tn(z, sh)
        upd[0, m:m + B, :] = (low + (tn(x, sm) + tn(y, sh))) + tn(x, sh)


def finish(a_red, g_red, a_old, s_old, s_inv):
    f32 = jnp.float32
    full = pl.BlockSpec((1, D, D), lambda l: (l, 0, 0))
    shape = jax.ShapeDtypeStruct((L, D, D), f32)
    return pl.pallas_call(
        finish_kernel,
        grid=(L,),
        in_specs=[
            pl.BlockSpec((1, DEV, AR, D), lambda l: (l, 0, 0, 0)),
            pl.BlockSpec((1, DEV, SR, D), lambda l: (L - 1 - l, 0, 0, 0)),
            full, full, full,
        ],
        out_specs=[full] * 3,
        out_shape=[shape] * 3,
        compiler_params=pltpu.CompilerParams(vmem_limit_bytes=60 * 2 ** 20),
        cost_estimate=pl.CostEstimate(flops=L * 12 * D ** 3, bytes_accessed=160 * 2 ** 20, transcendentals=0),
        name="kfac_finish",
    )(a_red, g_red, a_old, s_old, s_inv)


def solution(mesh):
    batch_axes = ('node', 'data')
    row_spec = P(batch_axes, None)
    full_spec = P()

    def kfac_step(tokens, grad_out, weights, a_old, s_old, a_inv, s_inv):
        inv_total = 1.0 / tokens.shape[0]

        def per_device(tok, dout, w, a_prev, s_prev, a_pre, s_pre):
            _, a_red, g_red = run_stack(tok, dout, w, a_pre, inv_total)
            return tuple(finish(a_red, g_red, a_prev, s_prev, s_pre))

        return jax.shard_map(per_device, mesh=mesh, in_specs=(row_spec, row_spec, full_spec, full_spec, full_spec, full_spec, full_spec), out_specs=(full_spec, full_spec, full_spec), check_vma=False)(tokens, grad_out, weights, a_old, s_old, a_inv, s_inv)

    return kfac_step
```

```python
import functools
import jax
import jax.numpy as jnp
from jax import lax
from jax.experimental import pallas as pl
from jax.experimental.pallas import tpu as pltpu
from jax.sharding import PartitionSpec as P

FACTOR_DECAY = 0.8
GELU_SCALE = 0.7978845608028654
GELU_CUBIC = 0.044715
D = 768
B = 256
H = 128
NT = 8
DEV = 8
AR = 48
GR = 96
SR = AR + GR
L = 8
MESH = pl.DeviceIdType.MESH
T1, T2, T3, T4, T5, T6, T7 = 0, 1, 0, 4, 2, 2, 4


def tn(left, right):
    return lax.dot_general(left, right, (((0,), (0,)), ((), ())), preferred_element_type=jnp.float32)


def nt(left, right):
    return lax.dot_general(left, right, (((1,), (1,)), ((), ())), preferred_element_type=jnp.float32)


def half_parts(half_act):
    y = half_act.astype(jnp.float32)
    sq = jnp.minimum(y * y, 1e37)
    kp = (8.0 * GELU_SCALE * GELU_CUBIC) * sq
    a = 2.0 * GELU_SCALE + kp
    return y, kp, a, jnp.tanh(y * a)


def gelu_value(half_act):
    y, _, _, t = half_parts(half_act)
    return (y + y * t).astype(jnp.bfloat16)


def gelu_both(half_act):
    y, kp, a, t = half_parts(half_act)
    opt = 1.0 + t
    h = y * opt
    slope2 = opt + (h * (1.0 - t)) * ((a + kp) + kp)
    return h.astype(jnp.bfloat16), slope2


def add_rows(acc, p, base, rows, first, c0, val):
    n = val.shape[0]
    r = first
    while r < first + n:
        d, o = divmod(r, rows)
        k = min(rows - o, first + n - r)
        acc[p, d, base + o:base + o + k, c0:c0 + val.shape[1]] += val[r - first:r - first + k, :]
        r += k


def set_rows(acc, q, first, c0, val):
    r = first
    while r < first + val.shape[0]:
        d, o = divmod(r, AR)
        k = min(AR - o, first + val.shape[0] - r)
        acc[q, d, o:o + k, c0:c0 + val.shape[1]] = val[r - first:r - first + k, :]
        r += k


def gram_add(acc, dg, p, x):
    top = tn(x[:, 0:B], x)
    dg[0] += top[:, 0:B]
    add_rows(acc, p, 0, AR, 0, B, top[:, B:])
    mid = tn(x[:, B:2 * B], x[:, B:])
    dg[1] += mid[:, 0:B]
    add_rows(acc, p, 0, AR, B, 0, mid[0:H, B:])
    add_rows(acc, p, 0, AR, B, B, mid[H:, B:])
    dg[2] += tn(x[:, 2 * B:], x[:, 2 * B:])


def row_col(n):
    return lax.broadcasted_iota(jnp.int32, (n, n), 0), lax.broadcasted_iota(jnp.int32, (n, n), 1)


def pack_diag(acc, ex, dg, q):
    r, c = row_col(B)
    rh, ch = row_col(H)
    d0, d1, d2 = dg[0], dg[1], dg[2]
    set_rows(acc, q, 0, 0, jnp.where(c >= r, d0, d1))
    set_rows(acc, q, B, 2 * B, jnp.where(ch >= rh, d2[0:H, 0:H], d2[H:, H:]))
    set_rows(acc, q, B, 2 * B + H, d2[0:H, H:])
    v1 = jnp.sum(jnp.where(c == r, d1, 0.0), axis=0, keepdims=True)
    v2 = jnp.sum(jnp.where(ch == rh, d2[H:, H:], 0.0), axis=0, keepdims=True)
    ex[q, :, 0:B] = jnp.broadcast_to(v1, (8, B))
    ex[q, :, B:B + H] = jnp.broadcast_to(v2, (8, H))
    ex[q, :, B + H:] = jnp.zeros((8, D - B - H), jnp.float32)


def split3(x):
    hi = x.astype(jnp.bfloat16)
    r = x - hi.astype(jnp.float32)
    mid = r.astype(jnp.bfloat16)
    lo = (r - mid.astype(jnp.float32)).astype(jnp.bfloat16)
    return hi, mid, lo


def step_kernel(tile, inv_total, tok, dout, w_ref, ainv, y_hbm, a_out, g_out, ax_out, gx_out,
                buf, obuf, hbuf, ybuf, wh, acc, dg, ex, exr, r1, r2a, r2b, r3a, r3b, own, ainv_v,
                ssem, rsem, lsem, xsem, tsem, ysem, osem, asem):
    w = pl.program_id(0)
    t = pl.program_id(1)
    node = lax.axis_index('node')
    data = lax.axis_index('data')
    cy, cx, cc = node, data // 2, lax.rem(data, 2)
    partner = (cy, cx * 2 + 1 - cc)
    xn = (cy, (1 - cx) * 2 + cc)
    yn = (1 - cy, cx * 2 + cc)
    me = cy * 4 + cx * 2 + cc

    def chunk(yy, xx, c):
        return yy * 4 + xx * 2 + c

    @pl.when((w == 0) & (t == 0))
    def _():
        bar = pltpu.get_barrier_semaphore()
        for dev in (partner, xn, yn):
            pl.semaphore_signal(bar, inc=1, device_id=dev, device_id_type=MESH)
        pl.semaphore_wait(bar, 3)
        for i in range(NT):
            pltpu.make_async_copy(tok.at[pl.ds(i * tile, tile), :], buf.at[i], tsem.at[i]).start()

    def rcopy(src, dst, p, k, dev):
        return pltpu.make_async_remote_copy(src_ref=src, dst_ref=dst, send_sem=ssem.at[p, k], recv_sem=rsem.at[p, k],
                                            device_id=dev, device_id_type=MESH)

    def stages(rows, out, xout, idx2, idx3, idx4, bwd):
        hh = rows // 2

        def c1(p, q):
            return [rcopy(acc.at[q, chunk(i // 2, i % 2, 1 - cc), pl.ds(0, rows)], r1.at[p, i, pl.ds(0, rows)], p, i, partner)
                    for i in range(4)] + [rcopy(ex.at[q], exr.at[p, 0], p, 20, partner)]

        def c2(p, q):
            a = [rcopy(acc.at[q, chunk(i, 1 - cx, cc), pl.ds(0, hh)], r2a.at[p, i, pl.ds(0, hh)], p, 4 + i, xn) for i in range(2)]
            b = [rcopy(acc.at[q, chunk(1 - cy, i, cc), pl.ds(hh, hh)], r2b.at[p, i, pl.ds(0, hh)], p, 6 + i, yn) for i in range(2)]
            return a + b + [rcopy(ex.at[q], exr.at[p, 1], p, 21, xn)]

        def c3(p, q):
            return [rcopy(acc.at[q, chunk(1 - cy, cx, cc), pl.ds(0, hh)], r3a.at[p, pl.ds(0, hh)], p, 8, yn),
                    rcopy(acc.at[q, chunk(cy, 1 - cx, cc), pl.ds(hh, hh)], r3b.at[p, pl.ds(0, hh)], p, 9, xn),
                    rcopy(ex.at[q], exr.at[p, 2], p, 22, yn)]

        def c4(p, idx):
            return [rcopy(own.at[p, pl.ds(0, hh)], out.at[idx, me, pl.ds(0, hh)], p, 10, yn),
                    rcopy(own.at[p, pl.ds(hh, hh)], out.at[idx, me, pl.ds(hh, hh)], p, 11, xn)]

        def keep(p, idx):
            return pltpu.make_async_copy(own.at[p, pl.ds(0, rows)], out.at[idx, me], lsem.at[p])

        def keep_x(p, q, idx):
            return pltpu.make_async_copy(ex.at[q], xout.at[idx], xsem.at[p])

        def c5(p, idx):
            def mv(d, o, k, dev):
                ref = out.at[idx, d, pl.ds(o, hh)]
                return rcopy(ref, ref, p, k, dev)
            a = [mv(chunk(i, cx, cc), 0, 12 + i, xn) for i in range(2)]
            b = [mv(chunk(cy, i, cc), hh, 14 + i, yn) for i in range(2)]
            return a + b

        def c6(p, idx):
            refs = [out.at[idx, chunk(i // 2, i % 2, cc)] for i in range(4)]
            return [rcopy(refs[i], refs[i], p, 16 + i, partner) for i in range(4)]

        def start(cs):
            for c in cs:
                c.start()

        def wait(cs):
            for c in cs:
                c.wait()

        def reduce1():
            pack_diag(acc, ex, dg, q1)
            start(c1(p1, q1))

        def reduce2():
            wait(c1(p1, q1))
            ex[q1] += exr[p1, 0]
            for i in range(4):
                acc[q1, chunk(i // 2, i % 2, cc), 0:rows, :] += r1[p1, i, 0:rows, :]
            start(c2(p1, q1))

        def reduce3():
            wait(c2(p2, q2))
            ex[q2] += exr[p2, 1]
            for i in range(2):
                acc[q2, chunk(i, cx, cc), 0:hh, :] += r2a[p2, i, 0:hh, :]
                acc[q2, chunk(cy, i, cc), hh:rows, :] += r2b[p2, i, 0:hh, :]
            start(c3(p2, q2))

        def reduce4():
            wait(c3(p2, q2))
            ex[q2] = (ex[q2] + exr[p2, 2]) * inv_total
            own[p2, 0:hh, :] = (acc[q2, me, 0:hh, :] + r3a[p2, 0:hh, :]) * inv_total
            own[p2, hh:rows, :] = (acc[q2, me, hh:rows, :] + r3b[p2, 0:hh, :]) * inv_total
            if bwd:
                pltpu.make_async_copy(ainv.at[L - 1 - idx2], ainv_v, asem).wait()
                gh, gm, gl = split3(own[p2, AR:SR, :])
                g3 = jnp.concatenate([gh, gm, gl], 0)
                g2 = jnp.concatenate([gh, gm], 0)
                for n in range(0, D, B):
                    ah, am, al = split3(ainv_v[n:n + B, :])
                    d1 = nt(g3, ah)
                    d2 = nt(g2, am)
                    d3 = nt(gh, al)
                    low = (d3 + d2[GR:, :]) + d1[2 * GR:, :]
                    own[p2, AR:SR, n:n + B] = (low + (d2[0:GR, :] + d1[GR:2 * GR, :])) + d1[0:GR, :]
            keep(p2, idx2).start()
            keep_x(p2, q2, idx2).start()
            start(c4(p2, idx2))

        def gather5():
            keep(p3, idx3).wait()
            keep_x(p3, q3, idx3).wait()
            wait(c4(p3, idx3))
            start(c5(p3, idx3))

        def gather6():
            wait(c5(p4, idx4))
            start(c6(p4, idx4))

        def gather7():
            wait(c6(p4, idx4))

        return reduce1, reduce2, reduce3, reduce4, gather5, gather6, gather7

    def at(cond, step, fn):
        pl.when(cond & (t == step))(fn)

    j1, j2, j3, j4 = w - 1, w - 2, w - 3, w - 4
    p1, p2, p3, p4 = lax.rem(w + 1, 2), lax.rem(w, 2), lax.rem(w + 1, 2), lax.rem(w, 2)
    q1, q2, q3 = lax.rem(w + 2, 3), lax.rem(w + 1, 3), lax.rem(w, 3)
    fw = stages(AR, a_out, ax_out, j2, j3, j4, False)
    bw = stages(SR, g_out, gx_out, j2 - L, j3 - L, j4 - L, True)
    is_f = [(j >= 0) & (j < L) for j in (j1, j2, j3, j4)]
    is_b = [(j >= L) & (j < 2 * L) for j in (j1, j2, j3, j4)]

    @pl.when(is_b[1] & (t == 0))
    def _():
        pltpu.make_async_copy(ainv.at[L - 1 - (j2 - L)], ainv_v, asem).start()

    for k, step, i in ((0, T1, 0), (2, T3, 1), (1, T2, 0), (5, T6, 3), (4, T5, 2), (3, T4, 1), (6, T7, 3)):
        at(is_f[i], step, fw[k])
        at(is_b[i], step, bw[k])

    p = lax.rem(w, 3)
    slot = lax.rem(t, 2)
    rs = min(tile, B)

    @pl.when((t == 0) & (w < 2 * L))
    def _():
        acc[p] = jnp.zeros(acc.shape[1:], jnp.float32)
        dg[...] = jnp.zeros_like(dg)
        wh[...] = w_ref[0] * jnp.bfloat16(0.5)

    @pl.when(w == 0)
    def _():
        pltpu.make_async_copy(tok.at[pl.ds(t * tile, tile), :], buf.at[t], tsem.at[t]).wait()

    def put_y(layer, i, s):
        return pltpu.make_async_copy(ybuf.at[s], y_hbm.at[layer, pl.ds(i * tile, tile), :], ysem.at[s])

    def get_y(layer, i, s):
        return pltpu.make_async_copy(y_hbm.at[layer, pl.ds(i * tile, tile), :], ybuf.at[s], ysem.at[s])

    def get_tok(i, s):
        return pltpu.make_async_copy(tok.at[pl.ds(i * tile, tile), :], ybuf.at[s], ysem.at[s])

    def put_o(i, s):
        return pltpu.make_async_copy(obuf.at[s], buf.at[i], osem.at[s])

    g_step = w * NT + t
    fwd_out = (g_step >= 2) & (g_step < (L - 1) * NT + 2)

    @pl.when(fwd_out)
    def _():
        put_y(0, 0, slot).wait()

    @pl.when(fwd_out | ((g_step >= L * NT + 2) & (g_step < (2 * L - 1) * NT + 2)))
    def _():
        put_o(0, slot).wait()

    @pl.when(w < L - 1)
    def _():
        x = buf.at[t]
        for r in range(0, tile, rs):
            for c in range(0, D, B):
                y = jnp.dot(x[r:r + rs, :], wh[:, c:c + B], preferred_element_type=jnp.float32).astype(jnp.bfloat16)
                ybuf[slot, r:r + rs, c:c + B] = y
                obuf[slot, r:r + rs, c:c + B] = gelu_value(y)
        gram_add(acc, dg, p, x[...])
        put_y(w, t, slot).start()
        put_o(t, slot).start()

    @pl.when(w == L - 1)
    def _():
        gram_add(acc, dg, p, buf[t])
        pltpu.make_async_copy(dout.at[pl.ds(t * tile, tile), :], buf.at[t], tsem.at[t]).start()

        @pl.when(t == NT - 1)
        def _():
            get_y(L - 2, 0, 0).start()

    @pl.when(w == L)
    def _():
        pltpu.make_async_copy(dout.at[pl.ds(t * tile, tile), :], buf.at[t], tsem.at[t]).wait()

    wn = jnp.where(t == NT - 1, w + 1, w)
    tn_ = jnp.where(t == NT - 1, 0, t + 1)

    @pl.when((w >= L) & (wn < 2 * L - 1))
    def _():
        get_y(2 * L - 2 - wn, tn_, 1 - slot).start()

    @pl.when((w >= L) & (wn == 2 * L - 1))
    def _():
        get_tok(tn_, 1 - slot).start()

    @pl.when((w >= L) & (w < 2 * L))
    def _():
        get_tok(0, slot).wait()

    def grad_add(g, h):
        for m in range(0, D, B):
            add_rows(acc, p, AR, GR, m, 0, tn(g[:, m:m + B], h))

    @pl.when((w >= L) & (w < 2 * L - 1))
    def _():
        g = buf.at[t]
        for r in range(0, tile, rs):
            for c in range(0, D, B):
                dh = nt(g[r:r + rs, :], wh[c:c + B, :]).astype(jnp.bfloat16)
                h, slope2 = gelu_both(ybuf[slot, r:r + rs, c:c + B])
                hbuf[r:r + rs, c:c + B] = h
                obuf[slot, r:r + rs, c:c + B] = (dh.astype(jnp.float32) * slope2).astype(jnp.bfloat16)
        gram_add(acc, dg, p, g[...])
        grad_add(g[...], hbuf[...])
        put_o(t, slot).start()

    @pl.when(w == 2 * L - 1)
    def _():
        g = buf[t]
        gram_add(acc, dg, p, g)
        grad_add(g, ybuf[slot])


def run_stack(tok, dout, w, a_inv, inv_total):
    n, d = tok.shape
    tile = n // NT
    f32, bf16 = jnp.float32, jnp.bfloat16
    any_spec = pl.BlockSpec(memory_space=pl.ANY)

    def w_map(i, t):
        return (jnp.where(i < L, i, jnp.clip(2 * L - 1 - i, 1, L - 1)), 0, 0)

    return pl.pallas_call(
        functools.partial(step_kernel, tile, inv_total),
        grid=(2 * L + 4, NT),
        in_specs=[any_spec, any_spec, pl.BlockSpec((1, d, d), w_map), any_spec],
        out_specs=[any_spec] * 5,
        out_shape=[
            jax.ShapeDtypeStruct((L - 1, n, d), bf16),
            jax.ShapeDtypeStruct((L, DEV, AR, d), f32),
            jax.ShapeDtypeStruct((L, DEV, SR, d), f32),
            jax.ShapeDtypeStruct((L, 8, d), f32),
            jax.ShapeDtypeStruct((L, 8, d), f32),
        ],
        scratch_shapes=[
            pltpu.VMEM((NT, tile, d), bf16),
            pltpu.VMEM((2, tile, d), bf16),
            pltpu.VMEM((tile, d), bf16),
            pltpu.VMEM((2, tile, d), bf16),
            pltpu.VMEM((d, d), bf16),
            pltpu.VMEM((3, DEV, SR, d), f32),
            pltpu.VMEM((3, B, B), f32),
            pltpu.VMEM((3, 8, d), f32),
            pltpu.VMEM((2, 3, 8, d), f32),
            pltpu.VMEM((2, 4, SR, d), f32),
            pltpu.VMEM((2, 2, SR // 2, d), f32),
            pltpu.VMEM((2, 2, SR // 2, d), f32),
            pltpu.VMEM((2, SR // 2, d), f32),
            pltpu.VMEM((2, SR // 2, d), f32),
            pltpu.VMEM((2, SR, d), f32),
            pltpu.VMEM((d, d), f32),
            pltpu.SemaphoreType.DMA((2, 23)),
            pltpu.SemaphoreType.DMA((2, 23)),
            pltpu.SemaphoreType.DMA((2,)),
            pltpu.SemaphoreType.DMA((2,)),
            pltpu.SemaphoreType.DMA((NT,)),
            pltpu.SemaphoreType.DMA((2,)),
            pltpu.SemaphoreType.DMA((2,)),
            pltpu.SemaphoreType.DMA,
        ],
        compiler_params=pltpu.CompilerParams(vmem_limit_bytes=67043328, collective_id=0, has_side_effects=True),
        cost_estimate=pl.CostEstimate(flops=2 * 33 * n * d * d, bytes_accessed=200 * 2 ** 20, transcendentals=0),
        name="kfac_stack",
    )(tok, dout, w, a_inv)


def finish_kernel(a_ref, g_ref, ax_ref, gx_ref, a_old, s_old, s_inv, upd, a_new, s_new):
    r, c = row_col(B)
    rh, ch = row_col(H)

    def unfold(p, x, old, new):
        def put(r0, c0, val):
            rs, cs = slice(r0, r0 + val.shape[0]), slice(c0, c0 + val.shape[1])
            new[0, rs, cs] = FACTOR_DECAY * old[0, rs, cs] + (1.0 - FACTOR_DECAY) * val

        def rows(first, n, c0, width):
            parts, k = [], first
            while k < first + n:
                d, o = divmod(k, AR)
                m = min(AR - o, first + n - k)
                parts.append(p[0, d, o:o + m, c0:c0 + width])
                k += m
            return jnp.concatenate(parts, 0)

        both = rows(0, B, 0, B)
        flip = both.T
        put(0, 0, jnp.where(c >= r, both, flip))
        put(B, B, jnp.where(c == r, x[0, 0:1, 0:B], jnp.where(c < r, both, flip)))
        for c0 in (B, 2 * B):
            blk = rows(0, B, c0, B)
            put(0, c0, blk)
            put(c0, 0, blk.T)
        for i in range(2):
            blk = rows(B, H, i * B, B)
            put(B + i * H, 2 * B, blk)
            put(2 * B, B + i * H, blk.T)
        both = rows(B, H, 2 * B, H)
        flip = both.T
        put(2 * B, 2 * B, jnp.where(ch >= rh, both, flip))
        put(2 * B + H, 2 * B + H, jnp.where(ch == rh, x[0, 0:1, B:B + H], jnp.where(ch < rh, both, flip)))
        blk = rows(B, H, 2 * B + H, H)
        put(2 * B, 2 * B + H, blk)
        put(2 * B + H, 2 * B, blk.T)

    unfold(a_ref, ax_ref, a_old, a_new)
    unfold(g_ref, gx_ref, s_old, s_new)
    sh, sm, sl = split3(s_inv[0])
    lt = jnp.concatenate([g_ref[0, d, AR:SR, :] for d in range(DEV)], 0)
    lh, lm, ll = split3(lt)
    for m in range(0, D, B):
        x, y, z = lh[:, m:m + B], lm[:, m:m + B], ll[:, m:m + B]
        low = (tn(y, sm) + tn(x, sl)) + tn(z, sh)
        upd[0, m:m + B, :] = (low + (tn(x, sm) + tn(y, sh))) + tn(x, sh)


def finish(a_red, g_red, a_ex, g_ex, a_old, s_old, s_inv):
    f32 = jnp.float32
    full = pl.BlockSpec((1, D, D), lambda l: (l, 0, 0))
    shape = jax.ShapeDtypeStruct((L, D, D), f32)
    return pl.pallas_call(
        finish_kernel,
        grid=(L,),
        in_specs=[
            pl.BlockSpec((1, DEV, AR, D), lambda l: (l, 0, 0, 0)),
            pl.BlockSpec((1, DEV, SR, D), lambda l: (L - 1 - l, 0, 0, 0)),
            pl.BlockSpec((1, 8, D), lambda l: (l, 0, 0)),
            pl.BlockSpec((1, 8, D), lambda l: (L - 1 - l, 0, 0)),
            full, full, full,
        ],
        out_specs=[full] * 3,
        out_shape=[shape] * 3,
        compiler_params=pltpu.CompilerParams(vmem_limit_bytes=60 * 2 ** 20),
        cost_estimate=pl.CostEstimate(flops=L * 12 * D ** 3, bytes_accessed=160 * 2 ** 20, transcendentals=0),
        name="kfac_finish",
    )(a_red, g_red, a_ex, g_ex, a_old, s_old, s_inv)


def solution(mesh):
    batch_axes = ('node', 'data')
    row_spec = P(batch_axes, None)
    full_spec = P()

    def kfac_step(tokens, grad_out, weights, a_old, s_old, a_inv, s_inv):
        inv_total = 1.0 / tokens.shape[0]

        def per_device(tok, dout, w, a_prev, s_prev, a_pre, s_pre):
            _, a_red, g_red, a_ex, g_ex = run_stack(tok, dout, w, a_pre, inv_total)
            return tuple(finish(a_red, g_red, a_ex, g_ex, a_prev, s_prev, s_pre))

        return jax.shard_map(per_device, mesh=mesh, in_specs=(row_spec, row_spec, full_spec, full_spec, full_spec, full_spec, full_spec), out_specs=(full_spec, full_spec, full_spec), check_vma=False)(tokens, grad_out, weights, a_old, s_old, a_inv, s_inv)

    return kfac_step
```

```python
import functools
import jax
import jax.numpy as jnp
from jax import lax
from jax.experimental import pallas as pl
from jax.experimental.pallas import tpu as pltpu
from jax.sharding import PartitionSpec as P

FACTOR_DECAY = 0.8
GELU_SCALE = 0.7978845608028654
GELU_CUBIC = 0.044715
D = 768
B = 256
H = 128
NT = 4
DEV = 8
AR = 48
GR = 96
SR = AR + GR
L = 8
MESH = pl.DeviceIdType.MESH
T1, T2, T3, T4, T5, T6, T7 = 0, 1, 3, 0, 3, 2, 3


def tn(left, right):
    return lax.dot_general(left, right, (((0,), (0,)), ((), ())), preferred_element_type=jnp.float32)


def nt(left, right):
    return lax.dot_general(left, right, (((1,), (1,)), ((), ())), preferred_element_type=jnp.float32)


def half_parts(half_act):
    y = half_act.astype(jnp.float32)
    sq = jnp.minimum(y * y, 1e37)
    kp = (8.0 * GELU_SCALE * GELU_CUBIC) * sq
    a = 2.0 * GELU_SCALE + kp
    return y, kp, a, jnp.tanh(y * a)


def gelu_value(half_act):
    y, _, _, t = half_parts(half_act)
    return (y + y * t).astype(jnp.bfloat16)


def gelu_both(half_act):
    y, kp, a, t = half_parts(half_act)
    opt = 1.0 + t
    h = y * opt
    slope2 = opt + (h * (1.0 - t)) * ((a + kp) + kp)
    return h.astype(jnp.bfloat16), slope2


def add_rows(acc, p, base, rows, first, c0, val):
    n = val.shape[0]
    r = first
    while r < first + n:
        d, o = divmod(r, rows)
        k = min(rows - o, first + n - r)
        acc[p, d, base + o:base + o + k, c0:c0 + val.shape[1]] += val[r - first:r - first + k, :]
        r += k


def set_rows(acc, q, first, c0, val):
    r = first
    while r < first + val.shape[0]:
        d, o = divmod(r, AR)
        k = min(AR - o, first + val.shape[0] - r)
        acc[q, d, o:o + k, c0:c0 + val.shape[1]] = val[r - first:r - first + k, :]
        r += k


def gram_add(acc, dg, p, x):
    top = tn(x[:, 0:B], x)
    dg[0] += top[:, 0:B]
    add_rows(acc, p, 0, AR, 0, B, top[:, B:])
    mid = tn(x[:, B:2 * B], x[:, B:])
    dg[1] += mid[:, 0:B]
    add_rows(acc, p, 0, AR, B, 0, mid[0:H, B:])
    add_rows(acc, p, 0, AR, B, B, mid[H:, B:])
    dg[2] += tn(x[:, 2 * B:], x[:, 2 * B:])


def row_col(n):
    return lax.broadcasted_iota(jnp.int32, (n, n), 0), lax.broadcasted_iota(jnp.int32, (n, n), 1)


def pack_diag(acc, ex, dg, q):
    r, c = row_col(B)
    rh, ch = row_col(H)
    d0, d1, d2 = dg[0], dg[1], dg[2]
    set_rows(acc, q, 0, 0, jnp.where(c >= r, d0, d1))
    set_rows(acc, q, B, 2 * B, jnp.where(ch >= rh, d2[0:H, 0:H], d2[H:, H:]))
    set_rows(acc, q, B, 2 * B + H, d2[0:H, H:])
    v1 = jnp.sum(jnp.where(c == r, d1, 0.0), axis=0, keepdims=True)
    v2 = jnp.sum(jnp.where(ch == rh, d2[H:, H:], 0.0), axis=0, keepdims=True)
    ex[q, :, 0:B] = jnp.broadcast_to(v1, (8, B))
    ex[q, :, B:B + H] = jnp.broadcast_to(v2, (8, H))
    ex[q, :, B + H:] = jnp.zeros((8, D - B - H), jnp.float32)


def split3(x):
    hi = x.astype(jnp.bfloat16)
    r = x - hi.astype(jnp.float32)
    mid = r.astype(jnp.bfloat16)
    lo = (r - mid.astype(jnp.float32)).astype(jnp.bfloat16)
    return hi, mid, lo


def step_kernel(tile, inv_total, tok, dout, w_ref, ainv, y_hbm, a_out, g_out, ax_out, gx_out,
                buf, obuf, hbuf, ybuf, wh, acc, dg, ex, exr, r1, r2a, r2b, r3a, r3b, own, ainv_v,
                ssem, rsem, lsem, xsem, tsem, ysem, osem, asem):
    w = pl.program_id(0)
    t = pl.program_id(1)
    node = lax.axis_index('node')
    data = lax.axis_index('data')
    cy, cx, cc = node, data // 2, lax.rem(data, 2)
    partner = (cy, cx * 2 + 1 - cc)
    xn = (cy, (1 - cx) * 2 + cc)
    yn = (1 - cy, cx * 2 + cc)
    me = cy * 4 + cx * 2 + cc

    def chunk(yy, xx, c):
        return yy * 4 + xx * 2 + c

    @pl.when((w == 0) & (t == 0))
    def _():
        bar = pltpu.get_barrier_semaphore()
        for dev in (partner, xn, yn):
            pl.semaphore_signal(bar, inc=1, device_id=dev, device_id_type=MESH)
        pl.semaphore_wait(bar, 3)
        for i in range(NT):
            pltpu.make_async_copy(tok.at[pl.ds(i * tile, tile), :], buf.at[i], tsem.at[i]).start()

    def rcopy(src, dst, p, k, dev):
        return pltpu.make_async_remote_copy(src_ref=src, dst_ref=dst, send_sem=ssem.at[p, k], recv_sem=rsem.at[p, k],
                                            device_id=dev, device_id_type=MESH)

    def stages(rows, out, xout, idx2, idx3, bwd):
        hh = rows // 2

        def c1(p, q):
            return [rcopy(acc.at[q, chunk(i // 2, i % 2, 1 - cc), pl.ds(0, rows)], r1.at[p, i, pl.ds(0, rows)], p, i, partner)
                    for i in range(4)] + [rcopy(ex.at[q], exr.at[p, 0], p, 20, partner)]

        def c2(p, q):
            a = [rcopy(acc.at[q, chunk(i, 1 - cx, cc), pl.ds(0, hh)], r2a.at[p, i, pl.ds(0, hh)], p, 4 + i, xn) for i in range(2)]
            b = [rcopy(acc.at[q, chunk(1 - cy, i, cc), pl.ds(hh, hh)], r2b.at[p, i, pl.ds(0, hh)], p, 6 + i, yn) for i in range(2)]
            return a + b + [rcopy(ex.at[q], exr.at[p, 1], p, 21, xn)]

        def c3(p, q):
            return [rcopy(acc.at[q, chunk(1 - cy, cx, cc), pl.ds(0, hh)], r3a.at[p, pl.ds(0, hh)], p, 8, yn),
                    rcopy(acc.at[q, chunk(cy, 1 - cx, cc), pl.ds(hh, hh)], r3b.at[p, pl.ds(0, hh)], p, 9, xn),
                    rcopy(ex.at[q], exr.at[p, 2], p, 22, yn)]

        def c4(p, idx):
            return [rcopy(own.at[p, pl.ds(0, hh)], out.at[idx, me, pl.ds(0, hh)], p, 10, yn),
                    rcopy(own.at[p, pl.ds(hh, hh)], out.at[idx, me, pl.ds(hh, hh)], p, 11, xn)]

        def keep(p, idx):
            return pltpu.make_async_copy(own.at[p, pl.ds(0, rows)], out.at[idx, me], lsem.at[p])

        def keep_x(p, q, idx):
            return pltpu.make_async_copy(ex.at[q], xout.at[idx], xsem.at[p])

        def c5(p, idx):
            def mv(d, o, k, dev):
                ref = out.at[idx, d, pl.ds(o, hh)]
                return rcopy(ref, ref, p, k, dev)
            a = [mv(chunk(i, cx, cc), 0, 12 + i, xn) for i in range(2)]
            b = [mv(chunk(cy, i, cc), hh, 14 + i, yn) for i in range(2)]
            return a + b

        def c6(p, idx):
            refs = [out.at[idx, chunk(i // 2, i % 2, cc)] for i in range(4)]
            return [rcopy(refs[i], refs[i], p, 16 + i, partner) for i in range(4)]

        def start(cs):
            for c in cs:
                c.start()

        def wait(cs):
            for c in cs:
                c.wait()

        def reduce1():
            pack_diag(acc, ex, dg, q1)
            start(c1(p1, q1))

        def reduce2():
            wait(c1(p1, q1))
            ex[q1] += exr[p1, 0]
            for i in range(4):
                acc[q1, chunk(i // 2, i % 2, cc), 0:rows, :] += r1[p1, i, 0:rows, :]
            start(c2(p1, q1))

        def reduce3():
            wait(c2(p1, q1))
            ex[q1] += exr[p1, 1]
            for i in range(2):
                acc[q1, chunk(i, cx, cc), 0:hh, :] += r2a[p1, i, 0:hh, :]
                acc[q1, chunk(cy, i, cc), hh:rows, :] += r2b[p1, i, 0:hh, :]
            start(c3(p1, q1))

        def reduce4():
            wait(c3(p2, q2))
            ex[q2] = (ex[q2] + exr[p2, 2]) * inv_total
            own[p2, 0:hh, :] = (acc[q2, me, 0:hh, :] + r3a[p2, 0:hh, :]) * inv_total
            own[p2, hh:rows, :] = (acc[q2, me, hh:rows, :] + r3b[p2, 0:hh, :]) * inv_total
            if bwd:
                pltpu.make_async_copy(ainv.at[L - 1 - idx2], ainv_v, asem).wait()
                gh, gm, gl = split3(own[p2, AR:SR, :])
                g3 = jnp.concatenate([gh, gm, gl], 0)
                g2 = jnp.concatenate([gh, gm], 0)
                for n in range(0, D, B):
                    ah, am, al = split3(ainv_v[n:n + B, :])
                    d1 = nt(g3, ah)
                    d2 = nt(g2, am)
                    d3 = nt(gh, al)
                    low = (d3 + d2[GR:, :]) + d1[2 * GR:, :]
                    own[p2, AR:SR, n:n + B] = (low + (d2[0:GR, :] + d1[GR:2 * GR, :])) + d1[0:GR, :]
            keep(p2, idx2).start()
            keep_x(p2, q2, idx2).start()
            start(c4(p2, idx2))

        def gather5():
            keep(p2, idx2).wait()
            keep_x(p2, q2, idx2).wait()
            wait(c4(p2, idx2))
            start(c5(p2, idx2))

        def gather6():
            wait(c5(p3, idx3))
            start(c6(p3, idx3))

        def gather7():
            wait(c6(p3, idx3))

        return reduce1, reduce2, reduce3, reduce4, gather5, gather6, gather7

    def at(cond, step, fn):
        pl.when(cond & (t == step))(fn)

    j1, j2, j3 = w - 1, w - 2, w - 3
    p1, p2, p3 = lax.rem(w + 1, 2), lax.rem(w, 2), lax.rem(w + 1, 2)
    q1, q2 = lax.rem(w + 2, 3), lax.rem(w + 1, 3)
    fw = stages(AR, a_out, ax_out, j2, j3, False)
    bw = stages(SR, g_out, gx_out, j2 - L, j3 - L, True)
    is_f = [(j >= 0) & (j < L) for j in (j1, j2, j3)]
    is_b = [(j >= L) & (j < 2 * L) for j in (j1, j2, j3)]

    @pl.when(is_b[0] & (t == 2))
    def _():
        pltpu.make_async_copy(ainv.at[L - 1 - (j1 - L)], ainv_v, asem).start()

    for k, step, i in ((0, T1, 0), (3, T4, 1), (1, T2, 0), (5, T6, 2), (2, T3, 0), (4, T5, 1), (6, T7, 2)):
        at(is_f[i], step, fw[k])
        at(is_b[i], step, bw[k])

    p = lax.rem(w, 3)
    slot = lax.rem(t, 2)
    rs = min(tile, B)

    @pl.when((t == 0) & (w < 2 * L))
    def _():
        acc[p] = jnp.zeros(acc.shape[1:], jnp.float32)
        dg[...] = jnp.zeros_like(dg)
        wh[...] = w_ref[0] * jnp.bfloat16(0.5)

    @pl.when(w == 0)
    def _():
        pltpu.make_async_copy(tok.at[pl.ds(t * tile, tile), :], buf.at[t], tsem.at[t]).wait()

    def put_y(layer, i, s):
        return pltpu.make_async_copy(ybuf.at[s], y_hbm.at[layer, pl.ds(i * tile, tile), :], ysem.at[s])

    def get_y(layer, i, s):
        return pltpu.make_async_copy(y_hbm.at[layer, pl.ds(i * tile, tile), :], ybuf.at[s], ysem.at[s])

    def get_tok(i, s):
        return pltpu.make_async_copy(tok.at[pl.ds(i * tile, tile), :], ybuf.at[s], ysem.at[s])

    def put_o(i, s):
        return pltpu.make_async_copy(obuf.at[s], buf.at[i], osem.at[s])

    g_step = w * NT + t
    fwd_out = (g_step >= 2) & (g_step < (L - 1) * NT + 2)

    @pl.when(fwd_out)
    def _():
        put_y(0, 0, slot).wait()

    @pl.when(fwd_out | ((g_step >= L * NT + 2) & (g_step < (2 * L - 1) * NT + 2)))
    def _():
        put_o(0, slot).wait()

    @pl.when(w < L - 1)
    def _():
        x = buf.at[t]
        for r in range(0, tile, rs):
            for c in range(0, D, B):
                y = jnp.dot(x[r:r + rs, :], wh[:, c:c + B], preferred_element_type=jnp.float32).astype(jnp.bfloat16)
                ybuf[slot, r:r + rs, c:c + B] = y
                obuf[slot, r:r + rs, c:c + B] = gelu_value(y)
        gram_add(acc, dg, p, x[...])
        put_y(w, t, slot).start()
        put_o(t, slot).start()

    @pl.when(w == L - 1)
    def _():
        gram_add(acc, dg, p, buf[t])
        pltpu.make_async_copy(dout.at[pl.ds(t * tile, tile), :], buf.at[t], tsem.at[t]).start()

        @pl.when(t == NT - 1)
        def _():
            get_y(L - 2, 0, 0).start()

    @pl.when(w == L)
    def _():
        pltpu.make_async_copy(dout.at[pl.ds(t * tile, tile), :], buf.at[t], tsem.at[t]).wait()

    wn = jnp.where(t == NT - 1, w + 1, w)
    tn_ = jnp.where(t == NT - 1, 0, t + 1)

    @pl.when((w >= L) & (wn < 2 * L - 1))
    def _():
        get_y(2 * L - 2 - wn, tn_, 1 - slot).start()

    @pl.when((w >= L) & (wn == 2 * L - 1))
    def _():
        get_tok(tn_, 1 - slot).start()

    @pl.when((w >= L) & (w < 2 * L))
    def _():
        get_tok(0, slot).wait()

    def grad_add(g, h):
        for m in range(0, D, B):
            add_rows(acc, p, AR, GR, m, 0, tn(g[:, m:m + B], h))

    @pl.when((w >= L) & (w < 2 * L - 1))
    def _():
        g = buf.at[t]
        for r in range(0, tile, rs):
            for c in range(0, D, B):
                dh = nt(g[r:r + rs, :], wh[c:c + B, :]).astype(jnp.bfloat16)
                h, slope2 = gelu_both(ybuf[slot, r:r + rs, c:c + B])
                hbuf[r:r + rs, c:c + B] = h
                obuf[slot, r:r + rs, c:c + B] = (dh.astype(jnp.float32) * slope2).astype(jnp.bfloat16)
        gram_add(acc, dg, p, g[...])
        grad_add(g[...], hbuf[...])
        put_o(t, slot).start()

    @pl.when(w == 2 * L - 1)
    def _():
        g = buf[t]
        gram_add(acc, dg, p, g)
        grad_add(g, ybuf[slot])


def run_stack(tok, dout, w, a_inv, inv_total):
    n, d = tok.shape
    tile = n // NT
    f32, bf16 = jnp.float32, jnp.bfloat16
    any_spec = pl.BlockSpec(memory_space=pl.ANY)

    def w_map(i, t):
        return (jnp.where(i < L, i, jnp.clip(2 * L - 1 - i, 1, L - 1)), 0, 0)

    return pl.pallas_call(
        functools.partial(step_kernel, tile, inv_total),
        grid=(2 * L + 3, NT),
        in_specs=[any_spec, any_spec, pl.BlockSpec((1, d, d), w_map), any_spec],
        out_specs=[any_spec] * 5,
        out_shape=[
            jax.ShapeDtypeStruct((L - 1, n, d), bf16),
            jax.ShapeDtypeStruct((L, DEV, AR, d), f32),
            jax.ShapeDtypeStruct((L, DEV, SR, d), f32),
            jax.ShapeDtypeStruct((L, 8, d), f32),
            jax.ShapeDtypeStruct((L, 8, d), f32),
        ],
        scratch_shapes=[
            pltpu.VMEM((NT, tile, d), bf16),
            pltpu.VMEM((2, tile, d), bf16),
            pltpu.VMEM((tile, d), bf16),
            pltpu.VMEM((2, tile, d), bf16),
            pltpu.VMEM((d, d), bf16),
            pltpu.VMEM((3, DEV, SR, d), f32),
            pltpu.VMEM((3, B, B), f32),
            pltpu.VMEM((3, 8, d), f32),
            pltpu.VMEM((2, 3, 8, d), f32),
            pltpu.VMEM((2, 4, SR, d), f32),
            pltpu.VMEM((2, 2, SR // 2, d), f32),
            pltpu.VMEM((2, 2, SR // 2, d), f32),
            pltpu.VMEM((2, SR // 2, d), f32),
            pltpu.VMEM((2, SR // 2, d), f32),
            pltpu.VMEM((2, SR, d), f32),
            pltpu.VMEM((d, d), f32),
            pltpu.SemaphoreType.DMA((2, 23)),
            pltpu.SemaphoreType.DMA((2, 23)),
            pltpu.SemaphoreType.DMA((2,)),
            pltpu.SemaphoreType.DMA((2,)),
            pltpu.SemaphoreType.DMA((NT,)),
            pltpu.SemaphoreType.DMA((2,)),
            pltpu.SemaphoreType.DMA((2,)),
            pltpu.SemaphoreType.DMA,
        ],
        compiler_params=pltpu.CompilerParams(vmem_limit_bytes=67043328, collective_id=0, has_side_effects=True),
        cost_estimate=pl.CostEstimate(flops=2 * 33 * n * d * d, bytes_accessed=200 * 2 ** 20, transcendentals=0),
        name="kfac_stack",
    )(tok, dout, w, a_inv)


def finish_kernel(a_ref, g_ref, ax_ref, gx_ref, a_old, s_old, s_inv, upd, a_new, s_new):
    r, c = row_col(B)
    rh, ch = row_col(H)

    def unfold(p, x, old, new):
        def put(r0, c0, val):
            rs, cs = slice(r0, r0 + val.shape[0]), slice(c0, c0 + val.shape[1])
            new[0, rs, cs] = FACTOR_DECAY * old[0, rs, cs] + (1.0 - FACTOR_DECAY) * val

        def rows(first, n, c0, width):
            parts, k = [], first
            while k < first + n:
                d, o = divmod(k, AR)
                m = min(AR - o, first + n - k)
                parts.append(p[0, d, o:o + m, c0:c0 + width])
                k += m
            return jnp.concatenate(parts, 0)

        both = rows(0, B, 0, B)
        flip = both.T
        put(0, 0, jnp.where(c >= r, both, flip))
        put(B, B, jnp.where(c == r, x[0, 0:1, 0:B], jnp.where(c < r, both, flip)))
        for c0 in (B, 2 * B):
            blk = rows(0, B, c0, B)
            put(0, c0, blk)
            put(c0, 0, blk.T)
        for i in range(2):
            blk = rows(B, H, i * B, B)
            put(B + i * H, 2 * B, blk)
            put(2 * B, B + i * H, blk.T)
        both = rows(B, H, 2 * B, H)
        flip = both.T
        put(2 * B, 2 * B, jnp.where(ch >= rh, both, flip))
        put(2 * B + H, 2 * B + H, jnp.where(ch == rh, x[0, 0:1, B:B + H], jnp.where(ch < rh, both, flip)))
        blk = rows(B, H, 2 * B + H, H)
        put(2 * B, 2 * B + H, blk)
        put(2 * B + H, 2 * B, blk.T)

    unfold(a_ref, ax_ref, a_old, a_new)
    unfold(g_ref, gx_ref, s_old, s_new)
    sh, sm, sl = split3(s_inv[0])
    lt = jnp.concatenate([g_ref[0, d, AR:SR, :] for d in range(DEV)], 0)
    lh, lm, ll = split3(lt)
    for m in range(0, D, B):
        x, y, z = lh[:, m:m + B], lm[:, m:m + B], ll[:, m:m + B]
        low = (tn(y, sm) + tn(x, sl)) + tn(z, sh)
        upd[0, m:m + B, :] = (low + (tn(x, sm) + tn(y, sh))) + tn(x, sh)


def finish(a_red, g_red, a_ex, g_ex, a_old, s_old, s_inv):
    f32 = jnp.float32
    full = pl.BlockSpec((1, D, D), lambda l: (l, 0, 0))
    shape = jax.ShapeDtypeStruct((L, D, D), f32)
    return pl.pallas_call(
        finish_kernel,
        grid=(L,),
        in_specs=[
            pl.BlockSpec((1, DEV, AR, D), lambda l: (l, 0, 0, 0)),
            pl.BlockSpec((1, DEV, SR, D), lambda l: (L - 1 - l, 0, 0, 0)),
            pl.BlockSpec((1, 8, D), lambda l: (l, 0, 0)),
            pl.BlockSpec((1, 8, D), lambda l: (L - 1 - l, 0, 0)),
            full, full, full,
        ],
        out_specs=[full] * 3,
        out_shape=[shape] * 3,
        compiler_params=pltpu.CompilerParams(vmem_limit_bytes=60 * 2 ** 20),
        cost_estimate=pl.CostEstimate(flops=L * 12 * D ** 3, bytes_accessed=160 * 2 ** 20, transcendentals=0),
        name="kfac_finish",
    )(a_red, g_red, a_ex, g_ex, a_old, s_old, s_inv)


def solution(mesh):
    batch_axes = ('node', 'data')
    row_spec = P(batch_axes, None)
    full_spec = P()

    def kfac_step(tokens, grad_out, weights, a_old, s_old, a_inv, s_inv):
        inv_total = 1.0 / tokens.shape[0]

        def per_device(tok, dout, w, a_prev, s_prev, a_pre, s_pre):
            _, a_red, g_red, a_ex, g_ex = run_stack(tok, dout, w, a_pre, inv_total)
            return tuple(finish(a_red, g_red, a_ex, g_ex, a_prev, s_prev, s_pre))

        return jax.shard_map(per_device, mesh=mesh, in_specs=(row_spec, row_spec, full_spec, full_spec, full_spec, full_spec, full_spec), out_specs=(full_spec, full_spec, full_spec), check_vma=False)(tokens, grad_out, weights, a_old, s_old, a_inv, s_inv)

    return kfac_step
```
